256 devices in a mesh: grp: 32 (over y, z_lo, core), dev: 8 (over x, z_hi).
Axes of the slice: x: 4, y: 4, z: 8 (z_hi: 2, z_lo: 4; z = z_hi * 4 + z_lo), core: 2. Of those that a mesh axis runs over, the one named last changes fastest.
Arguments:
- stack: bfloat16 [608, 256, 2048], P('grp', None, 'dev'), may hold values from -12 to 12
- network: int32 [608, 2], replicated, may hold values from 0 to 149, as said below
- bands: int32 [149], replicated, may hold values from 1 to 8
Outputs:
- deramped: bfloat16 [149, 256, 2048], P(None, 'grp', 'dev')
- misfit: float32 [256, 2048], P('grp', 'dev')
- spectrum: float32 [2, 149, 15, 15], replicated
The draws below stay inside these ranges and needn't reach their ends.
Inputs may be any that keep to these rules, and one draw needn't show every extreme that they name: `network`: each row holds a reference date and a later secondary date, both below 150; every pair of consecutive dates is some row.
All inputs are finite; a program needn't handle non-finite values.
Results may differ from the reference program's by a relative error of at most 0.005.
Values may be sent and summed in bfloat16 or wider, within the bound.
No kernel may reach another device: no remote copies, remote signals or barrier semaphores. Data moves between devices by JAX's collectives and lax.ppermute only.
A program may use at most 128 MiB of HBM per device.

```python
import math
import jax
import jax.numpy as jnp
from jax import lax

DATES = 150
IFGS = 608
ROW_DEV = 8
BAND = 8
SOLVED = 149
FREQS = 15
ROWS = 256
COLS = 2048


def draw_stack(key, part):
    first, second = jax.random.split(key, 2)
    noise = 1.5 * jax.random.truncated_normal(first, -4.0, 4.0, (IFGS, ROWS, COLS), jnp.float32)
    slopes = jax.random.uniform(second, (2, IFGS), jnp.float32, -6.0, 6.0)
    across = (jnp.arange(ROWS, dtype=jnp.float32) + 0.5) / ROWS - 0.5
    along = (jnp.arange(COLS, dtype=jnp.float32) + 0.5) / COLS - 0.5
    phase = noise + slopes[0][:, None, None] * across[None, :, None] + slopes[1][:, None, None] * along[None, None, :]
    return phase.astype(jnp.bfloat16)


def draw_network(key, part):
    first, second, third = jax.random.split(key, 3)
    extra = IFGS - (DATES - 1)
    chain_ref = jnp.arange(DATES - 1, dtype=jnp.int32)
    chain_sec = chain_ref + 1
    refs = jax.random.randint(first, (extra,), 0, DATES - 1, dtype=jnp.int32)
    gaps = jax.random.randint(second, (extra,), 0, DATES, dtype=jnp.int32)
    secs = refs + 1 + gaps % (DATES - 1 - refs)
    pairs = jnp.stack([jnp.concatenate([chain_ref, refs]), jnp.concatenate([chain_sec, secs])], axis=1)
    order = jax.random.permutation(third, IFGS)
    return pairs[order].astype(jnp.int32)


def set_ends(entries, stream_key, low, largest):
    extent = entries.shape
    index_at = [jax.random.randint(jax.random.fold_in(stream_key, axis), (), 0, extent[axis]) for axis in range(len(extent))]
    entries = entries.at[tuple(index_at)].set(low)
    longest = extent.index(max(extent))
    index_at[longest] = (index_at[longest] + 1) % extent[longest]
    return entries.at[tuple(index_at)].set(largest)


def setup_inputs(seed: int = 0) -> dict:
    splits = jax.random.split(jax.random.key(seed), 4)
    stack = draw_stack(jax.random.fold_in(splits[3], 71), 0)
    network = draw_network(jax.random.fold_in(splits[3], 71), 0)
    bands = set_ends(jax.random.randint(splits[2], (SOLVED,), 1, BAND + 1), jax.random.fold_in(splits[2], 1), 1, BAND).astype(jnp.int32)
    return {"stack": stack, "network": network, "bands": bands}


def build_inverse(network, solved):
    dates = jnp.arange(1, solved + 1, dtype=jnp.int32)
    design = (network[:, 1:2] == dates[None, :]).astype(jnp.float32) - (network[:, 0:1] == dates[None, :]).astype(jnp.float32)
    normal = jnp.dot(design.T, design, precision=lax.Precision.HIGHEST)
    factor = jnp.linalg.cholesky(normal)
    pinv = jax.scipy.linalg.cho_solve((factor, True), design.T)
    return (pinv.astype(jnp.bfloat16), design.astype(jnp.bfloat16))

def tables(positions, length, count):
    half = (count + 1) // 2
    steps = jnp.arange(count, dtype=jnp.int32) - (half - 1)
    turns = positions[:, None] * steps[None, :] % length
    angle = turns.astype(jnp.float32) * (2.0 * math.pi / length)
    return (jnp.cos(angle), jnp.sin(angle))

def reference(stack, network, bands):
    high = lax.Precision.HIGHEST
    pinv, design = build_inverse(network, SOLVED)
    blocks = ROWS // ROW_DEV

    def one_block(index):
        block = lax.dynamic_slice_in_dim(stack, (index * ROW_DEV).astype(jnp.int32), ROW_DEV, 1)
        flat = block.reshape(IFGS, ROW_DEV * COLS)
        series = jnp.dot(pinv.astype(jnp.float32), flat.astype(jnp.float32), preferred_element_type=jnp.float32)
        model = jnp.dot(design.astype(jnp.float32), series.astype(jnp.bfloat16).astype(jnp.float32), preferred_element_type=jnp.float32)
        resid = flat.astype(jnp.float32) - model
        misfit = jnp.sqrt(lax.optimization_barrier(jnp.mean(resid * resid, axis=0)) + 1e-06)
        return (series.reshape(SOLVED, ROW_DEV, COLS), misfit.reshape(ROW_DEV, COLS))
    series_blocks, misfit_blocks = lax.map(one_block, jnp.arange(blocks, dtype=jnp.int32))
    series = jnp.moveaxis(series_blocks, 0, 1).reshape(SOLVED, ROWS, COLS)
    misfit = misfit_blocks.reshape(ROWS, COLS)
    row_cos, row_sin = tables(jnp.arange(ROWS, dtype=jnp.int32), ROWS, FREQS)
    col_cos, col_sin = tables(jnp.arange(COLS, dtype=jnp.int32), COLS, FREQS)
    part_cos = jnp.einsum('thw,wl->thl', series, col_cos, precision=high)
    part_sin = jnp.einsum('thw,wl->thl', series, col_sin, precision=high)
    real = jnp.einsum('hk,thl->tkl', row_cos, part_cos, precision=high) - jnp.einsum('hk,thl->tkl', row_sin, part_sin, precision=high)
    imag = -(jnp.einsum('hk,thl->tkl', row_sin, part_cos, precision=high) + jnp.einsum('hk,thl->tkl', row_cos, part_sin, precision=high))
    scale = 1.0 / (ROWS * COLS)
    steps = jnp.abs(jnp.arange(FREQS, dtype=jnp.int32) - (BAND - 1))
    keep = (steps[None, :] < bands[:, None]).astype(jnp.float32)
    mask = keep[:, :, None] * keep[:, None, :]
    real = real * scale * mask
    imag = imag * scale * mask
    spectrum = jnp.stack([real, imag])
    rising = jnp.einsum('hk,tkl->thl', row_cos, real, precision=high) - jnp.einsum('hk,tkl->thl', row_sin, imag, precision=high)
    falling = -(jnp.einsum('hk,tkl->thl', row_sin, real, precision=high) + jnp.einsum('hk,tkl->thl', row_cos, imag, precision=high))
    ramp = jnp.einsum('thl,wl->thw', rising, col_cos, precision=high) + jnp.einsum('thl,wl->thw', falling, col_sin, precision=high)
    deramped = (series - ramp).astype(jnp.bfloat16)
    return (deramped, misfit, spectrum)
```

```python
import math

import jax
import jax.numpy as jnp
import numpy as np
from jax import lax
from jax.sharding import PartitionSpec as P

BAND = 8
FREQS = 2 * BAND - 1
HIGH = lax.Precision.HIGHEST


def design_of(network, solved):
    dates = jnp.arange(1, solved + 1, dtype=jnp.int32)
    return (network[:, 1:2] == dates[None, :]).astype(jnp.float32) - (
        network[:, 0:1] == dates[None, :]
    ).astype(jnp.float32)


def build_inverse(network, solved):
    design = design_of(network, solved)
    normal = jnp.dot(design.T, design, precision=HIGH)
    factor = jnp.linalg.cholesky(normal)
    pinv = jax.scipy.linalg.cho_solve((factor, True), design.T)
    return (pinv.astype(jnp.bfloat16), design.astype(jnp.bfloat16))


def basis(positions, length):
    index = jnp.arange(FREQS, dtype=jnp.int32)
    step = jnp.where(index < BAND, index, index - (BAND - 1))
    turns = positions[:, None] * step[None, :] % length
    angle = turns.astype(jnp.float32) * (2.0 * math.pi / length)
    return jnp.where(index[None, :] < BAND, jnp.cos(angle), jnp.sin(angle))


def mirror():
    out = np.zeros((FREQS, FREQS, 2, FREQS, FREQS), np.float32)
    for k in range(FREQS):
        for l in range(FREQS):
            fk, fl = k - (BAND - 1), l - (BAND - 1)
            ck, cl = abs(fk), abs(fl)
            sk, sl = abs(fk) + BAND - 1, abs(fl) + BAND - 1
            gk, gl = np.sign(fk), np.sign(fl)
            out[k, l, 0, ck, cl] += 1
            if gk * gl:
                out[k, l, 0, sk, sl] -= gk * gl
            if gk:
                out[k, l, 1, sk, cl] -= gk
            if gl:
                out[k, l, 1, ck, sl] -= gl
    return out.reshape(FREQS * FREQS * 2, FREQS * FREQS)


def on_device(stack, network, bands):
    solved = bands.shape[0]
    groups = lax.axis_size("grp")
    held, rows_all, col_dev = stack.shape
    row_dev = rows_all // groups
    cols_all = col_dev * lax.axis_size("dev")
    pixels = row_dev * col_dev

    packed = stack.reshape(held, groups, row_dev, col_dev).transpose(1, 0, 2, 3)
    block = lax.all_to_all(packed, "grp", 0, 0, tiled=True)

    rows = basis(jnp.arange(rows_all, dtype=jnp.int32), rows_all)
    cols = basis(
        lax.axis_index("dev") * col_dev + jnp.arange(col_dev, dtype=jnp.int32), cols_all
    )
    wide = stack.astype(jnp.float32)
    half = jnp.einsum("ihw,ha->iaw", wide, rows, precision=HIGH)
    local = jnp.einsum("iaw,wb->iab", half, cols, precision=HIGH)
    local = local.reshape(held, FREQS * FREQS)
    summed = lax.psum(local, "dev")
    every = lax.all_gather(summed, "grp", axis=0, tiled=True)

    pinv, design = build_inverse(network, solved)
    scale = 1.0 / (rows_all * cols_all)
    coef = scale * lax.dot_general(
        every, pinv.astype(jnp.float32), (((0,), (1,)), ((), ())), precision=HIGH
    )
    index = np.arange(FREQS)
    step = np.where(index < BAND, index, index - (BAND - 1))
    weight = np.where(step == 0, 1.0, 2.0)
    kmax = np.maximum(step[:, None], step[None, :]).reshape(-1)
    both = (weight[:, None] * weight[None, :]).reshape(-1).astype(np.float32)
    masked = jnp.where(jnp.asarray(kmax)[:, None] < bands[None, :], coef, 0.0)
    signed = jnp.dot(jnp.asarray(mirror()), masked, precision=HIGH)
    spectrum = signed.reshape(FREQS, FREQS, 2, solved).transpose(2, 3, 0, 1)

    row_here = basis(
        lax.axis_index("grp") * row_dev + jnp.arange(row_dev, dtype=jnp.int32), rows_all
    )
    waves = (row_here.T[:, None, :, None] * cols.T[None, :, None, :]).reshape(
        FREQS * FREQS, pixels
    )
    ramp = lax.dot_general(
        masked * jnp.asarray(both)[:, None], waves, (((0,), (0,)), ((), ())), precision=HIGH
    )

    flat = block.reshape(held * groups, pixels)
    series = jnp.dot(pinv, flat, preferred_element_type=jnp.float32)
    deramped = (series - ramp).astype(jnp.bfloat16).reshape(solved, row_dev, col_dev)
    model = jnp.dot(design, series.astype(jnp.bfloat16), preferred_element_type=jnp.float32)
    resid = flat.astype(jnp.float32) - model
    misfit = jnp.sqrt(jnp.mean(resid * resid, axis=0) + 1e-06).reshape(row_dev, col_dev)
    return (deramped, misfit, spectrum)


def solution(mesh):
    return jax.shard_map(
        on_device,
        mesh=mesh,
        in_specs=(P("grp", None, "dev"), P(), P()),
        out_specs=(P(None, "grp", "dev"), P("grp", "dev"), P()),
        check_vma=False,
    )
```

```python
import math

import jax
import jax.numpy as jnp
import numpy as np
from jax import lax
from jax.experimental import pallas as pl
from jax.experimental.pallas import tpu as pltpu
from jax.sharding import PartitionSpec as P


BAND = 8
FREQS = 2 * BAND - 1
HIGH = lax.Precision.HIGHEST


def design_of(network, solved):
    dates = jnp.arange(1, solved + 1, dtype=jnp.int32)
    return (network[:, 1:2] == dates[None, :]).astype(jnp.float32) - (
        network[:, 0:1] == dates[None, :]
    ).astype(jnp.float32)


def sweep_kernel(normal_ref, out_ref):
    size, width = out_ref.shape
    out_ref[...] = normal_ref[...]
    lane = lax.broadcasted_iota(jnp.int32, (size, width), 1)
    top = lax.broadcasted_iota(jnp.int32, (1, width), 1)

    def step(k, carry):
        whole = out_ref[...]
        row = out_ref[pl.ds(k, 1), :]
        col = jnp.sum(jnp.where(lane == k, whole, 0.0), axis=1, keepdims=True)
        pivot = jnp.sum(jnp.where(top == k, row, 0.0), axis=1, keepdims=True)
        inv = 1.0 / pivot
        scaled = jnp.where(top == k, inv, row * inv)
        out_ref[...] = jnp.where(lane == k, -col * inv, whole - col * scaled)
        out_ref[pl.ds(k, 1), :] = scaled
        return carry

    lax.fori_loop(0, size, step, 0)


def build_inverse(network, solved):
    design = design_of(network, solved).astype(jnp.bfloat16)
    normal = lax.dot_general(
        design, design, (((0,), (0,)), ((), ())), preferred_element_type=jnp.float32
    )
    size, width = -(-solved // 8) * 8, -(-solved // 128) * 128
    padded = jnp.pad(normal, ((0, size - solved), (0, width - solved)))
    at = jnp.arange(size)
    ones = jnp.where(at >= solved, 1.0, 0.0).astype(jnp.float32)
    padded = padded + jnp.where(at[:, None] == jnp.arange(width)[None, :], ones[:, None], 0.0)
    inverse = pl.pallas_call(
        sweep_kernel,
        out_shape=jax.ShapeDtypeStruct((size, width), jnp.float32),
        in_specs=[pl.BlockSpec(memory_space=pltpu.VMEM)],
        out_specs=pl.BlockSpec(memory_space=pltpu.VMEM),
        cost_estimate=pl.CostEstimate(
            flops=int(3e7), bytes_accessed=300000, transcendentals=0
        ),
        name="sweep",
    )(padded)[:solved, :solved]
    pinv = lax.dot_general(
        inverse, design.astype(jnp.float32), (((1,), (1,)), ((), ())), precision=HIGH
    )
    return (pinv.astype(jnp.bfloat16), design)


def basis(positions, length):
    index = jnp.arange(FREQS, dtype=jnp.int32)
    step = jnp.where(index < BAND, index, index - (BAND - 1))
    turns = positions[:, None] * step[None, :] % length
    angle = turns.astype(jnp.float32) * (2.0 * math.pi / length)
    return jnp.where(index[None, :] < BAND, jnp.cos(angle), jnp.sin(angle))


def mirror():
    out = np.zeros((FREQS, FREQS, 2, FREQS, FREQS), np.float32)
    for k in range(FREQS):
        for l in range(FREQS):
            fk, fl = k - (BAND - 1), l - (BAND - 1)
            ck, cl = abs(fk), abs(fl)
            sk, sl = abs(fk) + BAND - 1, abs(fl) + BAND - 1
            gk, gl = np.sign(fk), np.sign(fl)
            out[k, l, 0, ck, cl] += 1
            if gk * gl:
                out[k, l, 0, sk, sl] -= gk * gl
            if gk:
                out[k, l, 1, sk, cl] -= gk
            if gl:
                out[k, l, 1, ck, sl] -= gl
    return out.reshape(FREQS * FREQS * 2, FREQS * FREQS)


def swapped(value, grp_bits, dev_bits):
    devs = 8
    return lax.ppermute(
        value,
        ("grp", "dev"),
        [
            (g * devs + d, (g ^ grp_bits) * devs + (d ^ dev_bits))
            for g in range(32)
            for d in range(devs)
        ],
    )


def in_order(own, others, bit):
    place = lax.axis_index("grp") // bit % 4
    held = jnp.stack([own, *others])
    return held[place ^ jnp.arange(4)]


def share(local):
    near = [swapped(local, k << 1, 0) for k in (1, 2, 3)]
    far = [swapped(local, k << 1, 1) for k in (0, 1, 2, 3)]
    part = in_order(local, near, 2) + in_order(far[0], far[1:], 2)
    part = part + swapped(part, 0, 2)
    part = part + swapped(part, 0, 4)
    part = in_order(part, [swapped(part, k << 3, 0) for k in (1, 2, 3)], 8)
    other = swapped(part, 1, 0)
    first = lax.axis_index("grp") % 2 == 0
    both = jnp.stack([jnp.where(first, part, other), jnp.where(first, other, part)], axis=2)
    return both.reshape(-1, local.shape[-1])


def on_device(stack, network, bands):
    solved = bands.shape[0]
    groups = lax.axis_size("grp")
    held, rows_all, col_dev = stack.shape
    row_dev = rows_all // groups
    cols_all = col_dev * lax.axis_size("dev")
    pixels = row_dev * col_dev

    rows = basis(jnp.arange(rows_all, dtype=jnp.int32), rows_all)
    cols = basis(
        lax.axis_index("dev") * col_dev + jnp.arange(col_dev, dtype=jnp.int32), cols_all
    )
    wide = stack.astype(jnp.float32)
    half = jnp.einsum("ihw,ha->iaw", wide, rows, precision=HIGH)
    local = jnp.einsum("iaw,wb->iab", half, cols, precision=HIGH)
    local = local.reshape(held, FREQS * FREQS)

    packed = stack.reshape(held, groups, row_dev, col_dev).transpose(1, 0, 2, 3)
    packed, local = lax.optimization_barrier((packed, local))
    block = lax.all_to_all(packed, "grp", 0, 0, tiled=True)
    every = share(local)

    pinv, design = build_inverse(network, solved)
    scale = 1.0 / (rows_all * cols_all)
    coef = scale * lax.dot_general(
        every, pinv.astype(jnp.float32), (((0,), (1,)), ((), ())), precision=HIGH
    )
    index = np.arange(FREQS)
    step = np.where(index < BAND, index, index - (BAND - 1))
    weight = np.where(step == 0, 1.0, 2.0)
    kmax = np.maximum(step[:, None], step[None, :]).reshape(-1)
    both = (weight[:, None] * weight[None, :]).reshape(-1).astype(np.float32)
    masked = jnp.where(jnp.asarray(kmax)[:, None] < bands[None, :], coef, 0.0)
    signed = jnp.dot(jnp.asarray(mirror()), masked, precision=HIGH)
    spectrum = signed.reshape(FREQS, FREQS, 2, solved).transpose(2, 3, 0, 1)

    row_here = basis(
        lax.axis_index("grp") * row_dev + jnp.arange(row_dev, dtype=jnp.int32), rows_all
    )
    waves = (row_here.T[:, None, :, None] * cols.T[None, :, None, :]).reshape(
        FREQS * FREQS, pixels
    )
    ramp = lax.dot_general(
        masked * jnp.asarray(both)[:, None], waves, (((0,), (0,)), ((), ())), precision=HIGH
    )

    flat = block.reshape(held * groups, pixels)
    series = jnp.dot(pinv, flat, preferred_element_type=jnp.float32)
    deramped = (series - ramp).astype(jnp.bfloat16).reshape(solved, row_dev, col_dev)
    model = jnp.dot(design, series.astype(jnp.bfloat16), preferred_element_type=jnp.float32)
    resid = flat.astype(jnp.float32) - model
    misfit = jnp.sqrt(jnp.mean(resid * resid, axis=0) + 1e-06).reshape(row_dev, col_dev)
    return (deramped, misfit, spectrum)


def solution(mesh):
    return jax.shard_map(
        on_device,
        mesh=mesh,
        in_specs=(P("grp", None, "dev"), P(), P()),
        out_specs=(P(None, "grp", "dev"), P("grp", "dev"), P()),
        check_vma=False,
    )
```

```python
import math

import jax
import jax.numpy as jnp
import numpy as np
from jax import lax
from jax.experimental import pallas as pl
from jax.experimental.pallas import tpu as pltpu
from jax.sharding import PartitionSpec as P


BAND = 8
FREQS = 2 * BAND - 1
HIGH = lax.Precision.HIGHEST


def design_of(network, solved):
    dates = jnp.arange(1, solved + 1, dtype=jnp.int32)
    return (network[:, 1:2] == dates[None, :]).astype(jnp.float32) - (
        network[:, 0:1] == dates[None, :]
    ).astype(jnp.float32)


def sweep_kernel(normal_ref, out_ref):
    size, width = out_ref.shape
    out_ref[...] = normal_ref[...]
    lane = lax.broadcasted_iota(jnp.int32, (size, width), 1)
    top = lax.broadcasted_iota(jnp.int32, (1, width), 1)

    def pick(row, at):
        return jnp.sum(jnp.where(top == at, row, 0.0), axis=1, keepdims=True)

    def step(i, carry):
        k = 2 * i
        whole = out_ref[...]
        row0 = out_ref[pl.ds(k, 1), :]
        row1 = out_ref[pl.ds(k + 1, 1), :]
        first, second = lane == k, lane == k + 1
        col0 = jnp.sum(jnp.where(first, whole, 0.0), axis=1, keepdims=True)
        col1 = jnp.sum(jnp.where(second, whole, 0.0), axis=1, keepdims=True)
        p, q = pick(row0, k), pick(row0, k + 1)
        t, r = pick(row1, k), pick(row1, k + 1)
        inv = 1.0 / (p * r - q * t)
        row0 = jnp.where(top == k, 1.0, jnp.where(top == k + 1, 0.0, row0))
        row1 = jnp.where(top == k, 0.0, jnp.where(top == k + 1, 1.0, row1))
        new0 = (r * row0 - q * row1) * inv
        new1 = (p * row1 - t * row0) * inv
        rest = jnp.where(first | second, 0.0, whole)
        out_ref[...] = rest - col0 * new0 - col1 * new1
        out_ref[pl.ds(k, 1), :] = new0
        out_ref[pl.ds(k + 1, 1), :] = new1
        return carry

    lax.fori_loop(0, size // 2, step, 0)


def inverse_of(design):
    solved = design.shape[1]
    normal = lax.dot_general(
        design, design, (((0,), (0,)), ((), ())), preferred_element_type=jnp.float32
    )
    size, width = -(-solved // 8) * 8, -(-solved // 128) * 128
    padded = jnp.pad(normal, ((0, size - solved), (0, width - solved)))
    at = jnp.arange(size)
    ones = jnp.where(at >= solved, 1.0, 0.0).astype(jnp.float32)
    padded = padded + jnp.where(at[:, None] == jnp.arange(width)[None, :], ones[:, None], 0.0)
    inverse = pl.pallas_call(
        sweep_kernel,
        out_shape=jax.ShapeDtypeStruct((size, width), jnp.float32),
        in_specs=[pl.BlockSpec(memory_space=pltpu.VMEM)],
        out_specs=pl.BlockSpec(memory_space=pltpu.VMEM),
        cost_estimate=pl.CostEstimate(
            flops=int(3e7), bytes_accessed=300000, transcendentals=0
        ),
        name="sweep",
    )(padded)
    return inverse[:solved, :solved]


def basis(positions, length):
    index = jnp.arange(FREQS, dtype=jnp.int32)
    step = jnp.where(index < BAND, index, index - (BAND - 1))
    turns = positions[:, None] * step[None, :] % length
    angle = turns.astype(jnp.float32) * (2.0 * math.pi / length)
    return jnp.where(index[None, :] < BAND, jnp.cos(angle), jnp.sin(angle))


def mirror():
    out = np.zeros((FREQS, FREQS, 2, FREQS, FREQS), np.float32)
    for k in range(FREQS):
        for l in range(FREQS):
            fk, fl = k - (BAND - 1), l - (BAND - 1)
            ck, cl = abs(fk), abs(fl)
            sk, sl = abs(fk) + BAND - 1, abs(fl) + BAND - 1
            gk, gl = np.sign(fk), np.sign(fl)
            out[k, l, 0, ck, cl] += 1
            if gk * gl:
                out[k, l, 0, sk, sl] -= gk * gl
            if gk:
                out[k, l, 1, sk, cl] -= gk
            if gl:
                out[k, l, 1, ck, sl] -= gl
    return out.reshape(FREQS * FREQS * 2, FREQS * FREQS)


DEVS = 8
STAGED = 8


def permuted(value, move):
    pairs = []
    for g in range(32):
        for d in range(DEVS):
            to_g, to_d = move(g, d)
            pairs.append((g * DEVS + d, to_g * DEVS + to_d))
    return lax.ppermute(value, ("grp", "dev"), pairs)


def over_y(value, k):
    return permuted(value, lambda g, d: (g ^ (k << 3), d))


def over_z(value, k):
    return permuted(value, lambda g, d: (g ^ (k << 1), d))


def over_x(value, k):
    return permuted(value, lambda g, d: (g, d ^ (k << 1)))


def pick(value, at, axis):
    return lax.dynamic_index_in_dim(value, at, axis, keepdims=False)


def on_device(stack, network, bands):
    solved = bands.shape[0]
    grp, dev = lax.axis_index("grp"), lax.axis_index("dev")
    y, z, c, x = grp // 8, grp // 2 % 4, grp % 2, dev // 2
    groups = lax.axis_size("grp")
    held, rows_all, col_dev = stack.shape
    row_dev = rows_all // groups
    cols_all = col_dev * lax.axis_size("dev")
    pixels = row_dev * col_dev
    left = held - STAGED
    modes = FREQS * FREQS

    strips = stack.reshape(held, 4, 4, 2, row_dev, col_dev)
    early = strips[:STAGED]
    planes = [pick(early, z ^ k, 2).transpose(1, 2, 0, 3, 4) for k in range(4)]
    planes[1:] = [over_z(planes[k], k) for k in (1, 2, 3)]

    rows = basis(jnp.arange(rows_all, dtype=jnp.int32), rows_all)
    cols = basis(dev * col_dev + jnp.arange(col_dev, dtype=jnp.int32), cols_all)
    wide = stack.astype(jnp.float32)
    half = jnp.einsum("ihw,ha->iaw", wide, rows, precision=HIGH)
    local = jnp.einsum("iaw,wb->iab", half, cols, precision=HIGH)
    deep = -(-held // 8) * 8
    local = jnp.pad(local.reshape(held, modes), ((0, deep - held), (0, col_dev - modes)))
    local = local + over_x(local, 1)
    local = local + over_x(local, 2)
    near = permuted(local, lambda g, d: (g ^ (d // 2 << 1), d))
    far = permuted(local, lambda g, d: (g ^ (d // 2 << 1), d ^ 1))

    packed = strips[STAGED:].reshape(left, groups, row_dev, col_dev).transpose(1, 0, 2, 3)
    block = lax.all_to_all(packed, "grp", 0, 0, tiled=True)

    design = design_of(network, solved).astype(jnp.bfloat16)
    kc, ky, kz, j = np.meshgrid(
        np.arange(2), np.arange(4), np.arange(4), np.arange(STAGED), indexing="ij"
    )
    order_a = (((y ^ ky) * 4 + (z ^ kz)) * 2 + (c ^ kc)) * held + j
    order_b = np.arange(groups)[:, None] * held + np.arange(STAGED, held)[None, :]
    kc, ky, kr, j = np.meshgrid(
        np.arange(2), np.arange(4), np.arange(4), np.arange(deep), indexing="ij"
    )
    order_f = (((y ^ ky) * 4 + (z ^ x ^ kr)) * 2 + (c ^ kc)) * held + j
    order_f = jnp.where(j < held, order_f, -1)
    order = jnp.concatenate(
        [order_a.reshape(-1), jnp.asarray(order_b.reshape(-1)), order_f.reshape(-1)]
    )
    chosen = (order[:, None] == jnp.arange(held * groups)[None, :]).astype(jnp.bfloat16)
    sorted_design = jnp.dot(chosen, design, preferred_element_type=jnp.float32)
    inverse = inverse_of(design)
    pinv = lax.dot_general(
        inverse, sorted_design, (((1,), (1,)), ((), ())), precision=HIGH
    ).astype(jnp.bfloat16)
    cut_a, cut_b = groups * STAGED, groups * held
    pinv_a, pinv_b, pinv_f = pinv[:, :cut_a], pinv[:, cut_a:cut_b], pinv[:, cut_b:]
    sorted_design = sorted_design.astype(jnp.bfloat16)
    design_a, design_b = sorted_design[:cut_a], sorted_design[cut_a:cut_b]

    total = near + far
    total = jnp.stack([total, over_x(total, 1)])
    total = jnp.concatenate([total, over_x(total, 2)])
    high_part = total.astype(jnp.bfloat16)
    low_part = (total - high_part.astype(jnp.float32)).astype(jnp.bfloat16)
    sums = jnp.stack([high_part, low_part]).reshape(-1, row_dev, col_dev)
    count = sums.shape[0]

    def slabs(value):
        return value.reshape(-1, row_dev, col_dev)

    def toward(k):
        return jnp.stack([pick(p, y ^ k, 0) for p in planes])

    mine = toward(0)
    lines, shared = [mine], [sums]
    for k in (2, 1, 3):
        got = over_y(jnp.concatenate([slabs(toward(k)), sums]), k)
        lines.append(got[:-count].reshape(mine.shape))
        shared.append(got[-count:])
    lines = [lines[0], lines[2], lines[1], lines[3]]
    shared = [shared[0], shared[2], shared[1], shared[3]]
    shared = jnp.stack(shared)
    keep = jnp.stack([pick(p, c, 1) for p in lines])
    give = jnp.stack([pick(p, c ^ 1, 1) for p in lines])
    got = permuted(jnp.concatenate([slabs(give), slabs(shared)]), lambda g, d: (g ^ 1, d))
    part_a = jnp.concatenate([slabs(keep), got[: cut_a // 2]])
    shared = jnp.stack([shared.reshape(4, 2, 4 * deep, col_dev), got[cut_a // 2 :].reshape(4, 2, 4 * deep, col_dev)])

    scale = 1.0 / (rows_all * cols_all)

    def product(piece):
        return lax.dot_general(
            shared[:, :, piece].reshape(-1, col_dev),
            pinv_f,
            (((0,), (1,)), ((), ())),
            preferred_element_type=jnp.float32,
        )[:modes]

    coef = scale * (product(0) + product(1))
    index = np.arange(FREQS)
    step = np.where(index < BAND, index, index - (BAND - 1))
    weight = np.where(step == 0, 1.0, 2.0)
    kmax = np.maximum(step[:, None], step[None, :]).reshape(-1)
    both = (weight[:, None] * weight[None, :]).reshape(-1).astype(np.float32)
    masked = jnp.where(jnp.asarray(kmax)[:, None] < bands[None, :], coef, 0.0)
    signed = jnp.dot(jnp.asarray(mirror()), masked, precision=HIGH)
    spectrum = signed.reshape(FREQS, FREQS, 2, solved).transpose(2, 3, 0, 1)

    row_here = basis(grp * row_dev + jnp.arange(row_dev, dtype=jnp.int32), rows_all)
    waves = row_here.T[:, None, :, None] * cols.T[None, :, None, :]
    waves = waves.reshape(modes, pixels)
    ramp = lax.dot_general(
        masked * jnp.asarray(both)[:, None], waves, (((0,), (0,)), ((), ())), precision=HIGH
    )

    flat_a = part_a.reshape(-1, pixels)
    flat_b = block.reshape(-1, pixels)
    series = jnp.dot(pinv_a, flat_a, preferred_element_type=jnp.float32) + jnp.dot(
        pinv_b, flat_b, preferred_element_type=jnp.float32
    )
    deramped = (series - ramp).astype(jnp.bfloat16).reshape(solved, row_dev, col_dev)
    rounded = series.astype(jnp.bfloat16)
    energy = 0.0
    for flat, some in ((flat_a, design_a), (flat_b, design_b)):
        resid = flat.astype(jnp.float32) - jnp.dot(
            some, rounded, preferred_element_type=jnp.float32
        )
        energy = energy + jnp.sum(resid * resid, axis=0)
    misfit = jnp.sqrt(energy / (held * groups) + 1e-06).reshape(row_dev, col_dev)
    return (deramped, misfit, spectrum)


def solution(mesh):
    return jax.shard_map(
        on_device,
        mesh=mesh,
        in_specs=(P("grp", None, "dev"), P(), P()),
        out_specs=(P(None, "grp", "dev"), P("grp", "dev"), P()),
        check_vma=False,
    )
```

```python
import math

import jax
import jax.numpy as jnp
import numpy as np
from jax import lax
from jax.experimental import pallas as pl
from jax.experimental.pallas import tpu as pltpu
from jax.sharding import PartitionSpec as P


BAND = 8
FREQS = 2 * BAND - 1
HIGH = lax.Precision.HIGHEST


def design_of(network, solved):
    dates = jnp.arange(1, solved + 1, dtype=jnp.int32)
    return (network[:, 1:2] == dates[None, :]).astype(jnp.float32) - (
        network[:, 0:1] == dates[None, :]
    ).astype(jnp.float32)


def sweep_kernel(normal_ref, out_ref):
    size, width = out_ref.shape
    out_ref[...] = normal_ref[...]
    lane = lax.broadcasted_iota(jnp.int32, (size, width), 1)
    top = lax.broadcasted_iota(jnp.int32, (1, width), 1)

    def pick(row, at):
        return jnp.sum(jnp.where(top == at, row, 0.0), axis=1, keepdims=True)

    def step(i, carry):
        k = 2 * i
        whole = out_ref[...]
        row0 = out_ref[pl.ds(k, 1), :]
        row1 = out_ref[pl.ds(k + 1, 1), :]
        first, second = lane == k, lane == k + 1
        col0 = jnp.sum(jnp.where(first, whole, 0.0), axis=1, keepdims=True)
        col1 = jnp.sum(jnp.where(second, whole, 0.0), axis=1, keepdims=True)
        p, q = pick(row0, k), pick(row0, k + 1)
        t, r = pick(row1, k), pick(row1, k + 1)
        inv = 1.0 / (p * r - q * t)
        row0 = jnp.where(top == k, 1.0, jnp.where(top == k + 1, 0.0, row0))
        row1 = jnp.where(top == k, 0.0, jnp.where(top == k + 1, 1.0, row1))
        new0 = (r * row0 - q * row1) * inv
        new1 = (p * row1 - t * row0) * inv
        rest = jnp.where(first | second, 0.0, whole)
        out_ref[...] = rest - col0 * new0 - col1 * new1
        out_ref[pl.ds(k, 1), :] = new0
        out_ref[pl.ds(k + 1, 1), :] = new1
        return carry

    lax.fori_loop(0, size // 2, step, 0)


def inverse_of(design):
    solved = design.shape[1]
    normal = lax.dot_general(
        design, design, (((0,), (0,)), ((), ())), preferred_element_type=jnp.float32
    )
    size, width = -(-solved // 8) * 8, -(-solved // 128) * 128
    padded = jnp.pad(normal, ((0, size - solved), (0, width - solved)))
    at = jnp.arange(size)
    ones = jnp.where(at >= solved, 1.0, 0.0).astype(jnp.float32)
    padded = padded + jnp.where(at[:, None] == jnp.arange(width)[None, :], ones[:, None], 0.0)
    inverse = pl.pallas_call(
        sweep_kernel,
        out_shape=jax.ShapeDtypeStruct((size, width), jnp.float32),
        in_specs=[pl.BlockSpec(memory_space=pltpu.VMEM)],
        out_specs=pl.BlockSpec(memory_space=pltpu.VMEM),
        cost_estimate=pl.CostEstimate(
            flops=int(3e7), bytes_accessed=300000, transcendentals=0
        ),
        name="sweep",
    )(padded)
    return inverse[:solved, :solved]


def basis(positions, length):
    index = jnp.arange(FREQS, dtype=jnp.int32)
    step = jnp.where(index < BAND, index, index - (BAND - 1))
    turns = positions[:, None] * step[None, :] % length
    angle = turns.astype(jnp.float32) * (2.0 * math.pi / length)
    return jnp.where(index[None, :] < BAND, jnp.cos(angle), jnp.sin(angle))


def mirror():
    out = np.zeros((FREQS, FREQS, 2, FREQS, FREQS), np.float32)
    for k in range(FREQS):
        for l in range(FREQS):
            fk, fl = k - (BAND - 1), l - (BAND - 1)
            ck, cl = abs(fk), abs(fl)
            sk, sl = abs(fk) + BAND - 1, abs(fl) + BAND - 1
            gk, gl = np.sign(fk), np.sign(fl)
            out[k, l, 0, ck, cl] += 1
            if gk * gl:
                out[k, l, 0, sk, sl] -= gk * gl
            if gk:
                out[k, l, 1, sk, cl] -= gk
            if gl:
                out[k, l, 1, ck, sl] -= gl
    return out.reshape(FREQS * FREQS * 2, FREQS * FREQS)


DEVS = 8


def permuted(value, move):
    pairs = []
    for g in range(32):
        for d in range(DEVS):
            to_g, to_d = move(g, d)
            pairs.append((g * DEVS + d, to_g * DEVS + to_d))
    return lax.ppermute(value, ("grp", "dev"), pairs)


def over_y(value, k):
    return permuted(value, lambda g, d: (g ^ (k << 3), d))


def over_x(value, k):
    return permuted(value, lambda g, d: (g, d ^ (k << 1)))


def on_device(stack, network, bands):
    solved = bands.shape[0]
    grp, dev = lax.axis_index("grp"), lax.axis_index("dev")
    y, z, c, x = grp // 8, grp // 2 % 4, grp % 2, dev // 2
    groups = lax.axis_size("grp")
    held, rows_all, col_dev = stack.shape
    row_dev = rows_all // groups
    cols_all = col_dev * lax.axis_size("dev")
    modes = FREQS * FREQS
    ifgs = held * groups
    span = col_dev // 2

    strips = stack.reshape(held, groups, row_dev, col_dev)
    blocks = []
    for part in range(2):
        packed = strips[..., part * span : (part + 1) * span].transpose(1, 0, 2, 3)
        blocks.append(lax.all_to_all(packed, "grp", 0, 0, tiled=True))

    rows = basis(jnp.arange(rows_all, dtype=jnp.int32), rows_all)
    cols = basis(dev * col_dev + jnp.arange(col_dev, dtype=jnp.int32), cols_all)
    wide = stack.astype(jnp.float32)
    half = jnp.einsum("ihw,ha->iaw", wide, rows, precision=HIGH)
    local = jnp.einsum("iaw,wb->iab", half, cols, precision=HIGH)
    deep = -(-held // 8) * 8
    local = jnp.pad(local.reshape(held, modes), ((0, deep - held), (0, col_dev - modes)))
    local = local + over_x(local, 1)
    local = local + over_x(local, 2)
    near = permuted(local, lambda g, d: (g ^ (d // 2 << 1), d))
    far = permuted(local, lambda g, d: (g ^ (d // 2 << 1), d ^ 1))

    design = design_of(network, solved).astype(jnp.bfloat16)
    kc, ky, kr, j = np.meshgrid(
        np.arange(2), np.arange(4), np.arange(4), np.arange(deep), indexing="ij"
    )
    order = (((y ^ ky) * 4 + (z ^ x ^ kr)) * 2 + (c ^ kc)) * held + j
    order = jnp.where(j < held, order, -1).reshape(-1)
    inverse = inverse_of(design)
    pinv = lax.dot_general(
        inverse, design.astype(jnp.float32), (((1,), (1,)), ((), ())), precision=HIGH
    ).astype(jnp.bfloat16)
    chosen = (order[:, None] == jnp.arange(ifgs)[None, :]).astype(jnp.bfloat16)
    pinv_f = lax.dot_general(
        chosen, pinv, (((1,), (1,)), ((), ())), preferred_element_type=jnp.float32
    )

    total = near + far
    total = jnp.stack([total, over_x(total, 1)])
    total = jnp.concatenate([total, over_x(total, 2)]).reshape(-1, col_dev)
    lines = [over_y(total, k) for k in (1, 2, 3)]
    total = jnp.concatenate([total, *lines])
    other = permuted(total, lambda g, d: (g ^ 1, d))
    total = jnp.concatenate([total, other])

    scale = 1.0 / (rows_all * cols_all)
    coef = scale * lax.dot_general(
        total, pinv_f, (((0,), (0,)), ((), ())), precision=HIGH
    )[:modes]
    index = np.arange(FREQS)
    step = np.where(index < BAND, index, index - (BAND - 1))
    weight = np.where(step == 0, 1.0, 2.0)
    kmax = np.maximum(step[:, None], step[None, :]).reshape(-1)
    both = (weight[:, None] * weight[None, :]).reshape(-1).astype(np.float32)
    masked = jnp.where(jnp.asarray(kmax)[:, None] < bands[None, :], coef, 0.0)
    signed = jnp.dot(jnp.asarray(mirror()), masked, precision=HIGH)
    spectrum = signed.reshape(FREQS, FREQS, 2, solved).transpose(2, 3, 0, 1)
    weighed = masked * jnp.asarray(both)[:, None]
    row_here = basis(grp * row_dev + jnp.arange(row_dev, dtype=jnp.int32), rows_all)

    images, misfits = [], []
    for part, block in enumerate(blocks):
        here = cols[part * span : (part + 1) * span]
        waves = row_here.T[:, None, :, None] * here.T[None, :, None, :]
        ramp = lax.dot_general(
            weighed, waves.reshape(modes, -1), (((0,), (0,)), ((), ())), precision=HIGH
        )
        flat = block.reshape(ifgs, row_dev * span)
        series = jnp.dot(pinv, flat, preferred_element_type=jnp.float32)
        image = (series - ramp).astype(jnp.bfloat16)
        images.append(image.reshape(solved, row_dev, span))
        model = jnp.dot(design, series.astype(jnp.bfloat16), preferred_element_type=jnp.float32)
        resid = flat.astype(jnp.float32) - model
        misfit = jnp.sqrt(jnp.mean(resid * resid, axis=0) + 1e-06)
        misfits.append(misfit.reshape(row_dev, span))
    return (jnp.concatenate(images, axis=2), jnp.concatenate(misfits, axis=1), spectrum)


def solution(mesh):
    return jax.shard_map(
        on_device,
        mesh=mesh,
        in_specs=(P("grp", None, "dev"), P(), P()),
        out_specs=(P(None, "grp", "dev"), P("grp", "dev"), P()),
        check_vma=False,
    )
```

```python
import functools
import math

import jax
import jax.numpy as jnp
import numpy as np
from jax import lax
from jax.experimental import pallas as pl
from jax.experimental.pallas import tpu as pltpu
from jax.sharding import PartitionSpec as P


BAND = 8
FREQS = 2 * BAND - 1
HIGH = lax.Precision.HIGHEST


def design_of(network, solved):
    dates = jnp.arange(1, solved + 1, dtype=jnp.int32)
    return (network[:, 1:2] == dates[None, :]).astype(jnp.float32) - (
        network[:, 0:1] == dates[None, :]
    ).astype(jnp.float32)


def sweep_kernel(normal_ref, out_ref):
    size, width = out_ref.shape
    out_ref[...] = normal_ref[...]
    lane = lax.broadcasted_iota(jnp.int32, (size, width), 1)
    top = lax.broadcasted_iota(jnp.int32, (1, width), 1)

    def pick(row, at):
        return jnp.sum(jnp.where(top == at, row, 0.0), axis=1, keepdims=True)

    def step(i, carry):
        k = 2 * i
        whole = out_ref[...]
        row0 = out_ref[pl.ds(k, 1), :]
        row1 = out_ref[pl.ds(k + 1, 1), :]
        first, second = lane == k, lane == k + 1
        col0 = jnp.sum(jnp.where(first, whole, 0.0), axis=1, keepdims=True)
        col1 = jnp.sum(jnp.where(second, whole, 0.0), axis=1, keepdims=True)
        p, q = pick(row0, k), pick(row0, k + 1)
        t, r = pick(row1, k), pick(row1, k + 1)
        inv = 1.0 / (p * r - q * t)
        row0 = jnp.where(top == k, 1.0, jnp.where(top == k + 1, 0.0, row0))
        row1 = jnp.where(top == k, 0.0, jnp.where(top == k + 1, 1.0, row1))
        new0 = (r * row0 - q * row1) * inv
        new1 = (p * row1 - t * row0) * inv
        rest = jnp.where(first | second, 0.0, whole)
        out_ref[...] = rest - col0 * new0 - col1 * new1
        out_ref[pl.ds(k, 1), :] = new0
        out_ref[pl.ds(k + 1, 1), :] = new1
        return carry

    lax.fori_loop(0, size // 2, step, 0)


def inverse_of(design):
    solved = design.shape[1]
    normal = lax.dot_general(
        design, design, (((0,), (0,)), ((), ())), preferred_element_type=jnp.float32
    )
    size, width = -(-solved // 8) * 8, -(-solved // 128) * 128
    padded = jnp.pad(normal, ((0, size - solved), (0, width - solved)))
    at = jnp.arange(size)
    ones = jnp.where(at >= solved, 1.0, 0.0).astype(jnp.float32)
    padded = padded + jnp.where(at[:, None] == jnp.arange(width)[None, :], ones[:, None], 0.0)
    inverse = pl.pallas_call(
        sweep_kernel,
        out_shape=jax.ShapeDtypeStruct((size, width), jnp.float32),
        in_specs=[pl.BlockSpec(memory_space=pltpu.VMEM)],
        out_specs=pl.BlockSpec(memory_space=pltpu.VMEM),
        cost_estimate=pl.CostEstimate(
            flops=int(3e7), bytes_accessed=300000, transcendentals=0
        ),
        name="sweep",
    )(padded)
    return inverse[:solved, :solved]


def basis(positions, length):
    index = jnp.arange(FREQS, dtype=jnp.int32)
    step = jnp.where(index < BAND, index, index - (BAND - 1))
    turns = positions[:, None] * step[None, :] % length
    angle = turns.astype(jnp.float32) * (2.0 * math.pi / length)
    return jnp.where(index[None, :] < BAND, jnp.cos(angle), jnp.sin(angle))


def mirror():
    out = np.zeros((FREQS, FREQS, 2, FREQS, FREQS), np.float32)
    for k in range(FREQS):
        for l in range(FREQS):
            fk, fl = k - (BAND - 1), l - (BAND - 1)
            ck, cl = abs(fk), abs(fl)
            sk, sl = abs(fk) + BAND - 1, abs(fl) + BAND - 1
            gk, gl = np.sign(fk), np.sign(fl)
            out[k, l, 0, ck, cl] += 1
            if gk * gl:
                out[k, l, 0, sk, sl] -= gk * gl
            if gk:
                out[k, l, 1, sk, cl] -= gk
            if gl:
                out[k, l, 1, ck, sl] -= gl
    return out.transpose(2, 0, 1, 3, 4).reshape(2, FREQS * FREQS, FREQS * FREQS)


DEVS = 8


def permuted(value, move):
    pairs = []
    for g in range(32):
        for d in range(DEVS):
            to_g, to_d = move(g, d)
            pairs.append((g * DEVS + d, to_g * DEVS + to_d))
    return lax.ppermute(value, ("grp", "dev"), pairs)


def over_y(value, k):
    return permuted(value, lambda g, d: (g ^ (k << 3), d))


def over_x(value, k):
    return permuted(value, lambda g, d: (g, d ^ (k << 1)))


def pack_kernel(part, strips_ref, out_ref, sems):
    held, span = out_ref.shape[1], out_ref.shape[3]
    copies = [
        pltpu.make_async_copy(
            strips_ref.at[i, :, :, pl.ds(part * span, span)], out_ref.at[:, i], sems.at[i]
        )
        for i in range(held)
    ]
    for copy in copies:
        copy.start()
    for copy in copies:
        copy.wait()


def pack(strips, part, span):
    held, groups, row_dev, _ = strips.shape
    return pl.pallas_call(
        functools.partial(pack_kernel, part),
        out_shape=jax.ShapeDtypeStruct((groups, held, row_dev, span), strips.dtype),
        in_specs=[pl.BlockSpec(memory_space=pl.ANY)],
        out_specs=pl.BlockSpec(memory_space=pltpu.VMEM),
        scratch_shapes=[pltpu.SemaphoreType.DMA((held,))],
    )(strips)


def on_device(stack, network, bands):
    solved = bands.shape[0]
    grp, dev = lax.axis_index("grp"), lax.axis_index("dev")
    y, z, c, x = grp // 8, grp // 2 % 4, grp % 2, dev // 2
    groups = lax.axis_size("grp")
    held, rows_all, col_dev = stack.shape
    row_dev = rows_all // groups
    cols_all = col_dev * lax.axis_size("dev")
    modes = FREQS * FREQS
    ifgs = held * groups
    span = col_dev // 2

    strips = stack.reshape(held, groups, row_dev, col_dev)
    blocks = []
    for part in range(2):
        packed = pack(strips, part, span)
        blocks.append(lax.all_to_all(packed, "grp", 0, 0, tiled=True))

    rows = basis(jnp.arange(rows_all, dtype=jnp.int32), rows_all)
    cols = basis(dev * col_dev + jnp.arange(col_dev, dtype=jnp.int32), cols_all)
    wide = stack.astype(jnp.float32)
    half = jnp.einsum("ihw,ha->iaw", wide, rows, precision=HIGH)
    local = jnp.einsum("iaw,wb->iab", half, cols, precision=HIGH)
    deep = -(-held // 8) * 8
    local = jnp.pad(local.reshape(held, modes), ((0, deep - held), (0, col_dev - modes)))
    local = local + over_x(local, 1)
    local = local + over_x(local, 2)
    near = permuted(local, lambda g, d: (g ^ (d // 2 << 1), d))
    far = permuted(local, lambda g, d: (g ^ (d // 2 << 1), d ^ 1))

    design = design_of(network, solved).astype(jnp.bfloat16)
    kc, ky, kr, j = np.meshgrid(
        np.arange(2), np.arange(4), np.arange(4), np.arange(deep), indexing="ij"
    )
    order = (((y ^ ky) * 4 + (z ^ x ^ kr)) * 2 + (c ^ kc)) * held + j
    order = jnp.where(j < held, order, -1).reshape(-1)
    inverse = inverse_of(design)
    pinv = lax.dot_general(
        inverse, design.astype(jnp.float32), (((1,), (1,)), ((), ())), precision=HIGH
    ).astype(jnp.bfloat16)
    chosen = (order[:, None] == jnp.arange(ifgs)[None, :]).astype(jnp.bfloat16)
    pinv_f = lax.dot_general(
        chosen, pinv, (((1,), (1,)), ((), ())), preferred_element_type=jnp.float32
    )

    total = near + far
    total = jnp.stack([total, over_x(total, 1)])
    total = jnp.concatenate([total, over_x(total, 2)]).reshape(-1, col_dev)
    lines = [over_y(total, k) for k in (1, 2, 3)]
    total = jnp.concatenate([total, *lines])
    other = permuted(total, lambda g, d: (g ^ 1, d))
    total = jnp.concatenate([total, other])

    scale = 1.0 / (rows_all * cols_all)
    coef = scale * lax.dot_general(total, pinv_f, (((0,), (0,)), ((), ())), precision=HIGH)[:modes]
    index = np.arange(FREQS)
    step = np.where(index < BAND, index, index - (BAND - 1))
    weight = np.where(step == 0, 1.0, 2.0)
    kmax = np.maximum(step[:, None], step[None, :]).reshape(-1)
    both = (weight[:, None] * weight[None, :]).reshape(-1).astype(np.float32)
    masked = jnp.where(jnp.asarray(kmax)[:, None] < bands[None, :], coef, 0.0)
    signed = [jnp.dot(jnp.asarray(part), masked, precision=HIGH) for part in mirror()]
    spectrum = jnp.stack(signed).reshape(2, FREQS, FREQS, solved).transpose(0, 3, 1, 2)
    weighed = masked * jnp.asarray(both)[:, None]
    row_here = basis(grp * row_dev + jnp.arange(row_dev, dtype=jnp.int32), rows_all)

    images, misfits = [], []
    for part, block in enumerate(blocks):
        here = cols[part * span : (part + 1) * span]
        waves = row_here.T[:, None, :, None] * here.T[None, :, None, :]
        ramp = lax.dot_general(
            weighed, waves.reshape(modes, -1), (((0,), (0,)), ((), ())), precision=HIGH
        )
        flat = block.reshape(ifgs, row_dev * span)
        series = jnp.dot(pinv, flat, preferred_element_type=jnp.float32)
        image = (series - ramp).astype(jnp.bfloat16)
        images.append(image.reshape(solved, row_dev, span))
        model = jnp.dot(
            design, series.astype(jnp.bfloat16), preferred_element_type=jnp.float32
        )
        resid = flat.astype(jnp.float32) - model
        misfit = jnp.sqrt(jnp.mean(resid * resid, axis=0) + 1e-06)
        misfits.append(misfit.reshape(row_dev, span))
    return (jnp.concatenate(images, axis=2), jnp.concatenate(misfits, axis=1), spectrum)


def solution(mesh):
    return jax.shard_map(
        on_device,
        mesh=mesh,
        in_specs=(P("grp", None, "dev"), P(), P()),
        out_specs=(P(None, "grp", "dev"), P("grp", "dev"), P()),
        check_vma=False,
    )
```

```python
import math

import jax
import jax.numpy as jnp
import numpy as np
from jax import lax
from jax.experimental import pallas as pl
from jax.experimental.pallas import tpu as pltpu
from jax.sharding import PartitionSpec as P


BAND = 8
FREQS = 2 * BAND - 1
HIGH = lax.Precision.HIGHEST


def design_of(network, solved):
    dates = jnp.arange(1, solved + 1, dtype=jnp.int32)
    return (network[:, 1:2] == dates[None, :]).astype(jnp.float32) - (
        network[:, 0:1] == dates[None, :]
    ).astype(jnp.float32)


def sweep_kernel(normal_ref, out_ref):
    size, width = out_ref.shape
    out_ref[...] = normal_ref[...]
    lane = lax.broadcasted_iota(jnp.int32, (size, width), 1)
    top = lax.broadcasted_iota(jnp.int32, (1, width), 1)

    def pick(row, at):
        return jnp.sum(jnp.where(top == at, row, 0.0), axis=1, keepdims=True)

    def step(i, carry):
        k = 2 * i
        whole = out_ref[...]
        row0 = out_ref[pl.ds(k, 1), :]
        row1 = out_ref[pl.ds(k + 1, 1), :]
        first, second = lane == k, lane == k + 1
        col0 = jnp.sum(jnp.where(first, whole, 0.0), axis=1, keepdims=True)
        col1 = jnp.sum(jnp.where(second, whole, 0.0), axis=1, keepdims=True)
        p, q = pick(row0, k), pick(row0, k + 1)
        t, r = pick(row1, k), pick(row1, k + 1)
        inv = 1.0 / (p * r - q * t)
        row0 = jnp.where(top == k, 1.0, jnp.where(top == k + 1, 0.0, row0))
        row1 = jnp.where(top == k, 0.0, jnp.where(top == k + 1, 1.0, row1))
        new0 = (r * row0 - q * row1) * inv
        new1 = (p * row1 - t * row0) * inv
        rest = jnp.where(first | second, 0.0, whole)
        out_ref[...] = rest - col0 * new0 - col1 * new1
        out_ref[pl.ds(k, 1), :] = new0
        out_ref[pl.ds(k + 1, 1), :] = new1
        return carry

    lax.fori_loop(0, size // 2, step, 0)


def inverse_of(design):
    solved = design.shape[1]
    normal = lax.dot_general(
        design, design, (((0,), (0,)), ((), ())), preferred_element_type=jnp.float32
    )
    size, width = -(-solved // 8) * 8, -(-solved // 128) * 128
    padded = jnp.pad(normal, ((0, size - solved), (0, width - solved)))
    at = jnp.arange(size)
    ones = jnp.where(at >= solved, 1.0, 0.0).astype(jnp.float32)
    padded = padded + jnp.where(at[:, None] == jnp.arange(width)[None, :], ones[:, None], 0.0)
    inverse = pl.pallas_call(
        sweep_kernel,
        out_shape=jax.ShapeDtypeStruct((size, width), jnp.float32),
        in_specs=[pl.BlockSpec(memory_space=pltpu.VMEM)],
        out_specs=pl.BlockSpec(memory_space=pltpu.VMEM),
        cost_estimate=pl.CostEstimate(
            flops=int(3e7), bytes_accessed=300000, transcendentals=0
        ),
        name="sweep",
    )(padded)
    return inverse[:solved, :solved]


def basis(positions, length):
    index = jnp.arange(FREQS, dtype=jnp.int32)
    step = jnp.where(index < BAND, index, index - (BAND - 1))
    turns = positions[:, None] * step[None, :] % length
    angle = turns.astype(jnp.float32) * (2.0 * math.pi / length)
    return jnp.where(index[None, :] < BAND, jnp.cos(angle), jnp.sin(angle))


def mirror():
    out = np.zeros((FREQS, FREQS, 2, FREQS, FREQS), np.float32)
    for k in range(FREQS):
        for l in range(FREQS):
            fk, fl = k - (BAND - 1), l - (BAND - 1)
            ck, cl = abs(fk), abs(fl)
            sk, sl = abs(fk) + BAND - 1, abs(fl) + BAND - 1
            gk, gl = np.sign(fk), np.sign(fl)
            out[k, l, 0, ck, cl] += 1
            if gk * gl:
                out[k, l, 0, sk, sl] -= gk * gl
            if gk:
                out[k, l, 1, sk, cl] -= gk
            if gl:
                out[k, l, 1, ck, sl] -= gl
    return out.reshape(FREQS * FREQS * 2, FREQS * FREQS)


DEVS = 8


def permuted(value, move):
    pairs = []
    for g in range(32):
        for d in range(DEVS):
            to_g, to_d = move(g, d)
            pairs.append((g * DEVS + d, to_g * DEVS + to_d))
    return lax.ppermute(value, ("grp", "dev"), pairs)


def over_y(value, k):
    return permuted(value, lambda g, d: (g ^ (k << 3), d))


def over_z(value, k):
    return permuted(value, lambda g, d: (g ^ (k << 1), d))


def over_x(value, k):
    return permuted(value, lambda g, d: (g, d ^ (k << 1)))


HBM = pl.BlockSpec(memory_space=pl.ANY)


def copied(plan, scalars, arrays, shapes):
    def body(*refs):
        some, rest = refs[: len(scalars)], refs[len(scalars) :]
        ins, outs, sem = rest[: len(arrays)], rest[len(arrays) : -1], rest[-1]
        pairs = plan([ref[0] for ref in some], ins, outs)
        copies = [
            pltpu.make_async_copy(source, target, sem.at[i])
            for i, (source, target) in enumerate(pairs)
        ]
        for copy in copies:
            copy.start()
        for copy in copies:
            copy.wait()

    return pl.pallas_call(
        body,
        out_shape=[jax.ShapeDtypeStruct(shape, arrays[0].dtype) for shape in shapes],
        in_specs=[pl.BlockSpec(memory_space=pltpu.SMEM)] * len(scalars)
        + [HBM] * len(arrays),
        out_specs=[HBM] * len(shapes),
        scratch_shapes=[pltpu.SemaphoreType.DMA((32,))],
    )(*[jnp.reshape(v, (1,)) for v in scalars], *arrays)


def on_device(stack, network, bands):
    solved = bands.shape[0]
    grp, dev = lax.axis_index("grp"), lax.axis_index("dev")
    y, z, c, x = grp // 8, grp // 2 % 4, grp % 2, dev // 2
    groups = lax.axis_size("grp")
    held, rows_all, col_dev = stack.shape
    row_dev = rows_all // groups
    cols_all = col_dev * lax.axis_size("dev")
    modes = FREQS * FREQS
    ifgs = held * groups
    span = col_dev // 2
    tile = (row_dev, span)
    quad = 4 * held

    strips = stack.reshape(held, 4, 4, 2, row_dev, col_dev)

    def plane_plan(scalars, ins, outs):
        return [
            (ins[0].at[:, i, scalars[0] ^ k, j, :, pl.ds(0, span)], outs[k].at[i, j])
            for k in range(4)
            for i in range(4)
            for j in range(2)
        ]

    planes = copied(plane_plan, [z], [strips], [(4, 2, held, *tile)] * 4)
    planes = list(planes)
    planes[1:] = [over_z(planes[k], k) for k in (1, 2, 3)]

    rows = basis(jnp.arange(rows_all, dtype=jnp.int32), rows_all)
    cols = basis(dev * col_dev + jnp.arange(col_dev, dtype=jnp.int32), cols_all)
    wide = stack.astype(jnp.float32)
    half = jnp.einsum("ihw,ha->iaw", wide, rows, precision=HIGH)
    local = jnp.einsum("iaw,wb->iab", half, cols, precision=HIGH)
    deep = -(-held // 8) * 8
    local = jnp.pad(local.reshape(held, modes), ((0, deep - held), (0, col_dev - modes)))
    local = local + over_x(local, 1)
    local = local + over_x(local, 2)
    near = permuted(local, lambda g, d: (g ^ (d // 2 << 1), d))
    far = permuted(local, lambda g, d: (g ^ (d // 2 << 1), d ^ 1))

    def bulk_plan(scalars, ins, outs):
        return [
            (ins[0].at[i, :, :, pl.ds(span, span)], outs[0].at[:, i]) for i in range(held)
        ]

    (packed,) = copied(
        bulk_plan, [], [stack.reshape(held, groups, row_dev, col_dev)], [(groups, held, *tile)]
    )
    block = lax.all_to_all(packed, "grp", 0, 0, tiled=True)

    design = design_of(network, solved).astype(jnp.bfloat16)

    def arrival(plane, depth):
        kc, ky, kz, j = np.meshgrid(
            np.arange(2), np.arange(4), np.arange(4), np.arange(depth), indexing="ij"
        )
        order = (((y ^ ky) * 4 + (plane ^ kz)) * 2 + (c ^ kc)) * held + j
        return jnp.where(j < held, order, -1).reshape(-1)

    def one_hot(order):
        return (order[:, None] == jnp.arange(ifgs)[None, :]).astype(jnp.bfloat16)

    design_a = jnp.dot(
        one_hot(arrival(z, held)), design, preferred_element_type=jnp.float32
    ).astype(jnp.bfloat16)
    inverse = inverse_of(design)
    pinv, pinv_a = (
        lax.dot_general(
            inverse, some.astype(jnp.float32), (((1,), (1,)), ((), ())), precision=HIGH
        ).astype(jnp.bfloat16)
        for some in (design, design_a)
    )
    pinv_f = lax.dot_general(
        one_hot(arrival(z ^ x, deep)),
        pinv,
        (((1,), (1,)), ((), ())),
        preferred_element_type=jnp.float32,
    )

    total = near + far
    total = jnp.stack([total, over_x(total, 1)])
    total = jnp.concatenate([total, over_x(total, 2)]).reshape(4 * deep, 2, span)
    total = total.transpose(1, 0, 2)
    top = lax.reduce_precision(total, 8, 7)
    sums = jnp.stack([top, total - top]).astype(jnp.bfloat16).reshape(-1, *tile)
    count = sums.shape[0]

    def line_plan(scalars, ins, outs):
        pairs = [
            (ins[kz].at[scalars[0] ^ k, j], outs[k].at[pl.ds(j * quad + kz * held, held)])
            for k in range(4)
            for kz in range(4)
            for j in range(2)
        ]
        return pairs

    lines = copied(line_plan, [y], planes, [(2 * quad, *tile)] * 4)
    lines = [jnp.concatenate([line, sums]) for line in lines]
    lines[1:] = [over_y(lines[k], k) for k in (1, 2, 3)]

    def core_plan(scalars, ins, outs):
        keep, give = outs
        pairs = []
        for k in range(4):
            at = pl.ds(k * quad, quad)
            pairs.append((ins[k].at[pl.ds(scalars[0] * quad, quad)], keep.at[at]))
            pairs.append((ins[k].at[pl.ds((1 - scalars[0]) * quad, quad)], give.at[at]))
            pairs.append(
                (ins[k].at[pl.ds(2 * quad, count)], give.at[pl.ds(4 * quad + k * count, count)])
            )
        return pairs

    keep, give = copied(core_plan, [c], lines, [(4 * quad, *tile), (4 * quad + 4 * count, *tile)])
    got = permuted(give, lambda g, d: (g ^ 1, d))

    def combined(value):
        pieces = value[4 * quad :].reshape(4, 2, 2, 4 * deep, span).astype(jnp.float32)
        return (pieces[:, 0] + pieces[:, 1]).transpose(0, 2, 1, 3).reshape(-1, col_dev)

    total = jnp.concatenate([combined(give), combined(got)])
    scale = 1.0 / (rows_all * cols_all)
    coef = scale * lax.dot_general(total, pinv_f, (((0,), (0,)), ((), ())), precision=HIGH)[:modes]
    index = np.arange(FREQS)
    step = np.where(index < BAND, index, index - (BAND - 1))
    weight = np.where(step == 0, 1.0, 2.0)
    kmax = np.maximum(step[:, None], step[None, :]).reshape(-1)
    both = (weight[:, None] * weight[None, :]).reshape(-1).astype(np.float32)
    masked = jnp.where(jnp.asarray(kmax)[:, None] < bands[None, :], coef, 0.0)
    signed = jnp.dot(jnp.asarray(mirror()), masked, precision=HIGH)
    spectrum = signed.reshape(FREQS, FREQS, 2, solved).transpose(2, 3, 0, 1)
    weighed = masked * jnp.asarray(both)[:, None]
    row_here = basis(grp * row_dev + jnp.arange(row_dev, dtype=jnp.int32), rows_all)

    cut = 4 * quad
    first = [(keep, pinv_a[:, :cut], design_a[:cut]), (got[:cut], pinv_a[:, cut:], design_a[cut:])]
    images, misfits = [], []
    for part, pieces in enumerate((first, [(block, pinv, design)])):
        here = cols[part * span : (part + 1) * span]
        waves = row_here.T[:, None, :, None] * here.T[None, :, None, :]
        ramp = lax.dot_general(
            weighed, waves.reshape(modes, -1), (((0,), (0,)), ((), ())), precision=HIGH
        )
        series = 0.0
        for held_block, some_pinv, _ in pieces:
            flat = held_block.reshape(-1, row_dev * span)
            series = series + jnp.dot(some_pinv, flat, preferred_element_type=jnp.float32)
        image = (series - ramp).astype(jnp.bfloat16)
        images.append(image.reshape(solved, row_dev, span))
        energy = 0.0
        for held_block, _, some_design in pieces:
            flat = held_block.reshape(-1, row_dev * span)
            model = jnp.dot(
                some_design, series.astype(jnp.bfloat16), preferred_element_type=jnp.float32
            )
            resid = flat.astype(jnp.float32) - model
            energy = energy + jnp.sum(resid * resid, axis=0)
        misfit = jnp.sqrt(energy / ifgs + 1e-06)
        misfits.append(misfit.reshape(row_dev, span))
    return (jnp.concatenate(images, axis=2), jnp.concatenate(misfits, axis=1), spectrum)


def solution(mesh):
    return jax.shard_map(
        on_device,
        mesh=mesh,
        in_specs=(P("grp", None, "dev"), P(), P()),
        out_specs=(P(None, "grp", "dev"), P("grp", "dev"), P()),
        check_vma=False,
    )
```

```python
import math

import jax
import jax.numpy as jnp
import numpy as np
from jax import lax
from jax.experimental import pallas as pl
from jax.experimental.pallas import tpu as pltpu
from jax.sharding import PartitionSpec as P


BAND = 8
FREQS = 2 * BAND - 1
HIGH = lax.Precision.HIGHEST


def design_of(network, solved):
    dates = jnp.arange(1, solved + 1, dtype=jnp.int32)
    return (network[:, 1:2] == dates[None, :]).astype(jnp.float32) - (
        network[:, 0:1] == dates[None, :]
    ).astype(jnp.float32)


def sweep_kernel(normal_ref, out_ref):
    size, width = out_ref.shape
    out_ref[...] = normal_ref[...]
    lane = lax.broadcasted_iota(jnp.int32, (size, width), 1)
    top = lax.broadcasted_iota(jnp.int32, (1, width), 1)

    def pick(row, at):
        return jnp.sum(jnp.where(top == at, row, 0.0), axis=1, keepdims=True)

    def step(i, carry):
        k = 2 * i
        whole = out_ref[...]
        row0 = out_ref[pl.ds(k, 1), :]
        row1 = out_ref[pl.ds(k + 1, 1), :]
        first, second = lane == k, lane == k + 1
        col0 = jnp.sum(jnp.where(first, whole, 0.0), axis=1, keepdims=True)
        col1 = jnp.sum(jnp.where(second, whole, 0.0), axis=1, keepdims=True)
        p, q = pick(row0, k), pick(row0, k + 1)
        t, r = pick(row1, k), pick(row1, k + 1)
        inv = 1.0 / (p * r - q * t)
        row0 = jnp.where(top == k, 1.0, jnp.where(top == k + 1, 0.0, row0))
        row1 = jnp.where(top == k, 0.0, jnp.where(top == k + 1, 1.0, row1))
        new0 = (r * row0 - q * row1) * inv
        new1 = (p * row1 - t * row0) * inv
        rest = jnp.where(first | second, 0.0, whole)
        out_ref[...] = rest - col0 * new0 - col1 * new1
        out_ref[pl.ds(k, 1), :] = new0
        out_ref[pl.ds(k + 1, 1), :] = new1
        return carry

    lax.fori_loop(0, size // 2, step, 0)


def inverse_of(design):
    solved = design.shape[1]
    normal = lax.dot_general(
        design, design, (((0,), (0,)), ((), ())), preferred_element_type=jnp.float32
    )
    size, width = -(-solved // 8) * 8, -(-solved // 128) * 128
    padded = jnp.pad(normal, ((0, size - solved), (0, width - solved)))
    at = jnp.arange(size)
    ones = jnp.where(at >= solved, 1.0, 0.0).astype(jnp.float32)
    padded = padded + jnp.where(at[:, None] == jnp.arange(width)[None, :], ones[:, None], 0.0)
    inverse = pl.pallas_call(
        sweep_kernel,
        out_shape=jax.ShapeDtypeStruct((size, width), jnp.float32),
        in_specs=[pl.BlockSpec(memory_space=pltpu.VMEM)],
        out_specs=pl.BlockSpec(memory_space=pltpu.VMEM),
        cost_estimate=pl.CostEstimate(
            flops=int(3e7), bytes_accessed=300000, transcendentals=0
        ),
        name="sweep",
    )(padded)
    return inverse[:solved, :solved]


def basis(positions, length):
    index = jnp.arange(FREQS, dtype=jnp.int32)
    step = jnp.where(index < BAND, index, index - (BAND - 1))
    turns = positions[:, None] * step[None, :] % length
    angle = turns.astype(jnp.float32) * (2.0 * math.pi / length)
    return jnp.where(index[None, :] < BAND, jnp.cos(angle), jnp.sin(angle))


def mirror():
    out = np.zeros((FREQS, FREQS, 2, FREQS, FREQS), np.float32)
    for k in range(FREQS):
        for l in range(FREQS):
            fk, fl = k - (BAND - 1), l - (BAND - 1)
            ck, cl = abs(fk), abs(fl)
            sk, sl = abs(fk) + BAND - 1, abs(fl) + BAND - 1
            gk, gl = np.sign(fk), np.sign(fl)
            out[k, l, 0, ck, cl] += 1
            if gk * gl:
                out[k, l, 0, sk, sl] -= gk * gl
            if gk:
                out[k, l, 1, sk, cl] -= gk
            if gl:
                out[k, l, 1, ck, sl] -= gl
    return out.reshape(FREQS * FREQS * 2, FREQS * FREQS)


DEVS = 8


def permuted(value, move):
    pairs = []
    for g in range(32):
        for d in range(DEVS):
            to_g, to_d = move(g, d)
            pairs.append((g * DEVS + d, to_g * DEVS + to_d))
    return lax.ppermute(value, ("grp", "dev"), pairs)


def over_y(value, k):
    return permuted(value, lambda g, d: (g ^ (k << 3), d))


def over_z(value, k):
    return permuted(value, lambda g, d: (g ^ (k << 1), d))


def over_x(value, k):
    return permuted(value, lambda g, d: (g, d ^ (k << 1)))


def copied(plan, scalars, arrays, shapes, far=False):
    near = pl.BlockSpec(memory_space=pltpu.VMEM)

    def body(*refs):
        some, rest = refs[: len(scalars)], refs[len(scalars) :]
        ins, rest = rest[: len(arrays)], rest[len(arrays) :]
        outs, sems = rest[: len(shapes)], rest[len(shapes) :]
        pairs = plan([ref[0] for ref in some], ins, outs)
        if not far:
            for source, target in pairs:
                target[...] = source[...]
            return
        copies = [
            pltpu.make_async_copy(source, target, sems[0].at[i])
            for i, (source, target) in enumerate(pairs)
        ]
        for copy in copies:
            copy.start()
        for copy in copies:
            copy.wait()

    return list(
        pl.pallas_call(
            body,
            out_shape=[pltpu.VMEM(shape, arrays[0].dtype) for shape in shapes],
            in_specs=[pl.BlockSpec(memory_space=pltpu.SMEM)] * len(scalars)
            + [pl.BlockSpec(memory_space=pl.ANY) if far else near] * len(arrays),
            out_specs=[near] * len(shapes),
            scratch_shapes=[pltpu.SemaphoreType.DMA((32,))] if far else [],
        )(*[jnp.reshape(v, (1,)) for v in scalars], *arrays)
    )


def on_device(stack, network, bands):
    solved = bands.shape[0]
    grp, dev = lax.axis_index("grp"), lax.axis_index("dev")
    y, z, c, x = grp // 8, grp // 2 % 4, grp % 2, dev // 2
    groups = lax.axis_size("grp")
    held, rows_all, col_dev = stack.shape
    row_dev = rows_all // groups
    cols_all = col_dev * lax.axis_size("dev")
    modes = FREQS * FREQS
    ifgs = held * groups
    span = col_dev // 2
    tile = (row_dev, span)
    quad = 4 * held

    strips = stack.reshape(held, 4, 4, 2, row_dev, col_dev)

    def plane_plan(scalars, ins, outs):
        return [
            (ins[0].at[:, i, scalars[0] ^ k, j, :, pl.ds(0, span)], outs[k].at[i, j])
            for k in range(4)
            for i in range(4)
            for j in range(2)
        ]

    planes = copied(plane_plan, [z], [strips], [(4, 2, held, *tile)] * 4, True)
    planes[1:] = [over_z(planes[k], k) for k in (1, 2, 3)]

    rows = basis(jnp.arange(rows_all, dtype=jnp.int32), rows_all)
    cols = basis(dev * col_dev + jnp.arange(col_dev, dtype=jnp.int32), cols_all)
    wide = stack.astype(jnp.float32)
    half = jnp.einsum("ihw,ha->iaw", wide, rows, precision=HIGH)
    local = jnp.einsum("iaw,wb->iab", half, cols, precision=HIGH)
    deep = -(-held // 8) * 8
    local = jnp.pad(local.reshape(held, modes), ((0, deep - held), (0, col_dev - modes)))
    local = local + over_x(local, 1)
    local = local + over_x(local, 2)
    near = permuted(local, lambda g, d: (g ^ (d // 2 << 1), d))
    far = permuted(local, lambda g, d: (g ^ (d // 2 << 1), d ^ 1))

    def bulk_plan(scalars, ins, outs):
        return [
            (ins[0].at[i, :, :, pl.ds(span, span)], outs[0].at[:, i]) for i in range(held)
        ]

    (packed,) = copied(
        bulk_plan,
        [],
        [stack.reshape(held, groups, row_dev, col_dev)],
        [(groups, held, *tile)],
        True,
    )
    block = lax.all_to_all(packed, "grp", 0, 0, tiled=True)

    design = design_of(network, solved).astype(jnp.bfloat16)

    def arrival(plane, depth):
        kc, ky, kz, j = np.meshgrid(
            np.arange(2), np.arange(4), np.arange(4), np.arange(depth), indexing="ij"
        )
        order = (((y ^ ky) * 4 + (plane ^ kz)) * 2 + (c ^ kc)) * held + j
        return jnp.where(j < held, order, -1).reshape(-1)

    def one_hot(order):
        return (order[:, None] == jnp.arange(ifgs)[None, :]).astype(jnp.bfloat16)

    design_a = jnp.dot(
        one_hot(arrival(z, held)), design, preferred_element_type=jnp.float32
    ).astype(jnp.bfloat16)
    inverse = inverse_of(design)
    pinv, pinv_a = (
        lax.dot_general(
            inverse, some.astype(jnp.float32), (((1,), (1,)), ((), ())), precision=HIGH
        ).astype(jnp.bfloat16)
        for some in (design, design_a)
    )
    pinv_f = lax.dot_general(
        one_hot(arrival(z ^ x, deep)),
        pinv,
        (((1,), (1,)), ((), ())),
        preferred_element_type=jnp.float32,
    )

    total = near + far
    total = jnp.stack([total, over_x(total, 1)])
    total = jnp.concatenate([total, over_x(total, 2)]).reshape(4 * deep, 2, span)
    total = total.transpose(1, 0, 2)
    top = lax.reduce_precision(total, 8, 7)
    sums = jnp.stack([top, total - top]).astype(jnp.bfloat16).reshape(-1, *tile)
    count = sums.shape[0]

    def line_plan(scalars, ins, outs):
        pairs = [
            (ins[kz].at[scalars[0] ^ k, j], outs[k].at[pl.ds(j * quad + kz * held, held)])
            for k in range(4)
            for kz in range(4)
            for j in range(2)
        ]
        return pairs + [(ins[4], outs[k].at[pl.ds(2 * quad, count)]) for k in range(4)]

    lines = copied(line_plan, [y], [*planes, sums], [(2 * quad + count, *tile)] * 4)
    lines[1:] = [over_y(lines[k], k) for k in (1, 2, 3)]

    def core_plan(scalars, ins, outs):
        keep, give = outs
        pairs = []
        for k in range(4):
            at = pl.ds(k * quad, quad)
            pairs.append((ins[k].at[pl.ds(scalars[0] * quad, quad)], keep.at[at]))
            pairs.append((ins[k].at[pl.ds((1 - scalars[0]) * quad, quad)], give.at[at]))
            pairs.append(
                (ins[k].at[pl.ds(2 * quad, count)], give.at[pl.ds(4 * quad + k * count, count)])
            )
        return pairs

    keep, give = copied(core_plan, [c], lines, [(4 * quad, *tile), (4 * quad + 4 * count, *tile)])
    got = permuted(give, lambda g, d: (g ^ 1, d))

    def combined(value):
        pieces = value[4 * quad :].reshape(4, 2, 2, 4 * deep, span).astype(jnp.float32)
        return (pieces[:, 0] + pieces[:, 1]).transpose(0, 2, 1, 3).reshape(-1, col_dev)

    total = jnp.concatenate([combined(give), combined(got)])
    scale = 1.0 / (rows_all * cols_all)
    coef = scale * lax.dot_general(total, pinv_f, (((0,), (0,)), ((), ())), precision=HIGH)[:modes]
    index = np.arange(FREQS)
    step = np.where(index < BAND, index, index - (BAND - 1))
    weight = np.where(step == 0, 1.0, 2.0)
    kmax = np.maximum(step[:, None], step[None, :]).reshape(-1)
    both = (weight[:, None] * weight[None, :]).reshape(-1).astype(np.float32)
    masked = jnp.where(jnp.asarray(kmax)[:, None] < bands[None, :], coef, 0.0)
    signed = jnp.dot(jnp.asarray(mirror()), masked, precision=HIGH)
    spectrum = signed.reshape(FREQS, FREQS, 2, solved).transpose(2, 3, 0, 1)
    weighed = masked * jnp.asarray(both)[:, None]
    row_here = basis(grp * row_dev + jnp.arange(row_dev, dtype=jnp.int32), rows_all)

    cut = 4 * quad
    first = [(keep, pinv_a[:, :cut], design_a[:cut]), (got[:cut], pinv_a[:, cut:], design_a[cut:])]
    images, misfits = [], []
    for part, pieces in enumerate((first, [(block, pinv, design)])):
        here = cols[part * span : (part + 1) * span]
        waves = row_here.T[:, None, :, None] * here.T[None, :, None, :]
        ramp = lax.dot_general(
            weighed, waves.reshape(modes, -1), (((0,), (0,)), ((), ())), precision=HIGH
        )
        series = 0.0
        for held_block, some_pinv, _ in pieces:
            flat = held_block.reshape(-1, row_dev * span)
            series = series + jnp.dot(some_pinv, flat, preferred_element_type=jnp.float32)
        image = (series - ramp).astype(jnp.bfloat16)
        images.append(image.reshape(solved, row_dev, span))
        energy = 0.0
        for held_block, _, some_design in pieces:
            flat = held_block.reshape(-1, row_dev * span)
            model = jnp.dot(
                some_design, series.astype(jnp.bfloat16), preferred_element_type=jnp.float32
            )
            resid = flat.astype(jnp.float32) - model
            energy = energy + jnp.sum(resid * resid, axis=0)
        misfit = jnp.sqrt(energy / ifgs + 1e-06)
        misfits.append(misfit.reshape(row_dev, span))
    return (jnp.concatenate(images, axis=2), jnp.concatenate(misfits, axis=1), spectrum)


def solution(mesh):
    return jax.shard_map(
        on_device,
        mesh=mesh,
        in_specs=(P("grp", None, "dev"), P(), P()),
        out_specs=(P(None, "grp", "dev"), P("grp", "dev"), P()),
        check_vma=False,
    )
```

```python
import math

import jax
import jax.numpy as jnp
import numpy as np
from jax import lax
from jax.experimental import pallas as pl
from jax.experimental.pallas import tpu as pltpu
from jax.sharding import PartitionSpec as P


BAND = 8
FREQS = 2 * BAND - 1
HIGH = lax.Precision.HIGHEST


def design_of(network, solved):
    dates = jnp.arange(1, solved + 1, dtype=jnp.int32)
    return (network[:, 1:2] == dates[None, :]).astype(jnp.float32) - (
        network[:, 0:1] == dates[None, :]
    ).astype(jnp.float32)


def sweep_kernel(normal_ref, out_ref):
    size, width = out_ref.shape
    out_ref[...] = normal_ref[...]
    lane = lax.broadcasted_iota(jnp.int32, (size, width), 1)
    top = lax.broadcasted_iota(jnp.int32, (1, width), 1)

    def pick(row, at):
        return jnp.sum(jnp.where(top == at, row, 0.0), axis=1, keepdims=True)

    def step(i, carry):
        k = 2 * i
        whole = out_ref[...]
        row0 = out_ref[pl.ds(k, 1), :]
        row1 = out_ref[pl.ds(k + 1, 1), :]
        first, second = lane == k, lane == k + 1
        col0 = jnp.sum(jnp.where(first, whole, 0.0), axis=1, keepdims=True)
        col1 = jnp.sum(jnp.where(second, whole, 0.0), axis=1, keepdims=True)
        p, q = pick(row0, k), pick(row0, k + 1)
        t, r = pick(row1, k), pick(row1, k + 1)
        inv = 1.0 / (p * r - q * t)
        row0 = jnp.where(top == k, 1.0, jnp.where(top == k + 1, 0.0, row0))
        row1 = jnp.where(top == k, 0.0, jnp.where(top == k + 1, 1.0, row1))
        new0 = (r * row0 - q * row1) * inv
        new1 = (p * row1 - t * row0) * inv
        rest = jnp.where(first | second, 0.0, whole)
        out_ref[...] = rest - col0 * new0 - col1 * new1
        out_ref[pl.ds(k, 1), :] = new0
        out_ref[pl.ds(k + 1, 1), :] = new1
        return carry

    lax.fori_loop(0, size // 2, step, 0)


def inverse_of(design):
    solved = design.shape[1]
    normal = lax.dot_general(
        design, design, (((0,), (0,)), ((), ())), preferred_element_type=jnp.float32
    )
    size, width = -(-solved // 8) * 8, -(-solved // 128) * 128
    padded = jnp.pad(normal, ((0, size - solved), (0, width - solved)))
    at = jnp.arange(size)
    ones = jnp.where(at >= solved, 1.0, 0.0).astype(jnp.float32)
    padded = padded + jnp.where(at[:, None] == jnp.arange(width)[None, :], ones[:, None], 0.0)
    inverse = pl.pallas_call(
        sweep_kernel,
        out_shape=jax.ShapeDtypeStruct((size, width), jnp.float32),
        in_specs=[pl.BlockSpec(memory_space=pltpu.VMEM)],
        out_specs=pl.BlockSpec(memory_space=pltpu.VMEM),
        cost_estimate=pl.CostEstimate(
            flops=int(3e7), bytes_accessed=300000, transcendentals=0
        ),
        name="sweep",
    )(padded)
    return inverse[:solved, :solved]


def basis(positions, length):
    index = jnp.arange(FREQS, dtype=jnp.int32)
    step = jnp.where(index < BAND, index, index - (BAND - 1))
    turns = positions[:, None] * step[None, :] % length
    angle = turns.astype(jnp.float32) * (2.0 * math.pi / length)
    return jnp.where(index[None, :] < BAND, jnp.cos(angle), jnp.sin(angle))


def mirror():
    out = np.zeros((FREQS, FREQS, 2, FREQS, FREQS), np.float32)
    for k in range(FREQS):
        for l in range(FREQS):
            fk, fl = k - (BAND - 1), l - (BAND - 1)
            ck, cl = abs(fk), abs(fl)
            sk, sl = abs(fk) + BAND - 1, abs(fl) + BAND - 1
            gk, gl = np.sign(fk), np.sign(fl)
            out[k, l, 0, ck, cl] += 1
            if gk * gl:
                out[k, l, 0, sk, sl] -= gk * gl
            if gk:
                out[k, l, 1, sk, cl] -= gk
            if gl:
                out[k, l, 1, ck, sl] -= gl
    return out.reshape(FREQS * FREQS * 2, FREQS * FREQS)


DEVS = 8


def permuted(value, move):
    pairs = []
    for g in range(32):
        for d in range(DEVS):
            to_g, to_d = move(g, d)
            pairs.append((g * DEVS + d, to_g * DEVS + to_d))
    return lax.ppermute(value, ("grp", "dev"), pairs)


def over_y(value, k):
    return permuted(value, lambda g, d: (g ^ (k << 3), d))


def over_z(value, k):
    return permuted(value, lambda g, d: (g ^ (k << 1), d))


def over_x(value, k):
    return permuted(value, lambda g, d: (g, d ^ (k << 1)))


def copied(plan, scalars, arrays, shapes, far=False):
    near = pl.BlockSpec(memory_space=pltpu.VMEM)

    def body(*refs):
        some, rest = refs[: len(scalars)], refs[len(scalars) :]
        ins, rest = rest[: len(arrays)], rest[len(arrays) :]
        outs, sems = rest[: len(shapes)], rest[len(shapes) :]
        pairs = plan([ref[0] for ref in some], ins, outs)
        if not far:
            for source, target in pairs:
                target[...] = source[...]
            return
        copies = [
            pltpu.make_async_copy(source, target, sems[0].at[i])
            for i, (source, target) in enumerate(pairs)
        ]
        for copy in copies:
            copy.start()
        for copy in copies:
            copy.wait()

    return list(
        pl.pallas_call(
            body,
            out_shape=[pltpu.VMEM(shape, arrays[0].dtype) for shape in shapes],
            in_specs=[pl.BlockSpec(memory_space=pltpu.SMEM)] * len(scalars)
            + [pl.BlockSpec(memory_space=pl.ANY) if far else near] * len(arrays),
            out_specs=[near] * len(shapes),
            scratch_shapes=[pltpu.SemaphoreType.DMA((32,))] if far else [],
        )(*[jnp.reshape(v, (1,)) for v in scalars], *arrays)
    )


def on_device(stack, network, bands):
    solved = bands.shape[0]
    grp, dev = lax.axis_index("grp"), lax.axis_index("dev")
    y, z, c, x = grp // 8, grp // 2 % 4, grp % 2, dev // 2
    groups = lax.axis_size("grp")
    held, rows_all, col_dev = stack.shape
    row_dev = rows_all // groups
    cols_all = col_dev * lax.axis_size("dev")
    modes = FREQS * FREQS
    ifgs = held * groups
    span = col_dev // 2
    tile = (row_dev, span)
    quad = 4 * held

    strips = stack.reshape(held, 4, 4, 2, row_dev, col_dev)

    def plane_plan(scalars, ins, outs):
        return [
            (ins[0].at[:, i, scalars[0] ^ k, j, :, pl.ds(0, span)], outs[k].at[i, j])
            for k in range(4)
            for i in range(4)
            for j in range(2)
        ]

    planes = copied(plane_plan, [z], [strips], [(4, 2, held, *tile)] * 4, True)
    planes[1:] = [over_z(planes[k], k) for k in (1, 2, 3)]

    rows = basis(jnp.arange(rows_all, dtype=jnp.int32), rows_all)
    cols = basis(dev * col_dev + jnp.arange(col_dev, dtype=jnp.int32), cols_all)
    wide = stack.astype(jnp.float32)
    half = jnp.einsum("ihw,ha->iaw", wide, rows, precision=HIGH)
    local = jnp.einsum("iaw,wb->iab", half, cols, precision=HIGH)
    deep = -(-held // 8) * 8
    local = jnp.pad(local.reshape(held, modes), ((0, deep - held), (0, col_dev - modes)))
    local = local + over_x(local, 1)
    local = local + over_x(local, 2)
    near = permuted(local, lambda g, d: (g ^ (d // 2 << 1), d))
    far = permuted(local, lambda g, d: (g ^ (d // 2 << 1), d ^ 1))

    def bulk_plan(scalars, ins, outs):
        return [
            (ins[0].at[i, :, :, pl.ds(span, span)], outs[0].at[:, i]) for i in range(held)
        ]

    (packed,) = copied(
        bulk_plan,
        [],
        [stack.reshape(held, groups, row_dev, col_dev)],
        [(groups, held, *tile)],
        True,
    )
    block = lax.all_to_all(packed, "grp", 0, 0, tiled=True)

    design = design_of(network, solved).astype(jnp.bfloat16)

    def arrival(plane, depth):
        kc, ky, kz, j = np.meshgrid(
            np.arange(2), np.arange(4), np.arange(4), np.arange(depth), indexing="ij"
        )
        order = (((y ^ ky) * 4 + (plane ^ kz)) * 2 + (c ^ kc)) * held + j
        return jnp.where(j < held, order, -1).reshape(-1)

    def one_hot(order):
        return (order[:, None] == jnp.arange(ifgs)[None, :]).astype(jnp.bfloat16)

    design_a = jnp.dot(
        one_hot(arrival(z, held)), design, preferred_element_type=jnp.float32
    ).astype(jnp.bfloat16)
    inverse = inverse_of(design)
    pinv, pinv_a = (
        lax.dot_general(
            inverse, some.astype(jnp.float32), (((1,), (1,)), ((), ())), precision=HIGH
        ).astype(jnp.bfloat16)
        for some in (design, design_a)
    )
    pinv_f = lax.dot_general(
        one_hot(arrival(z ^ x, deep)),
        pinv,
        (((1,), (1,)), ((), ())),
        preferred_element_type=jnp.float32,
    )

    def line_plan(scalars, ins, outs):
        return [
            (ins[kz].at[scalars[0] ^ k, j], outs[k].at[pl.ds(j * quad + kz * held, held)])
            for k in range(4)
            for kz in range(4)
            for j in range(2)
        ]

    lines = copied(line_plan, [y], planes, [(2 * quad, *tile)] * 4)
    lines[1:] = [over_y(lines[k], k) for k in (1, 2, 3)]

    def core_plan(scalars, ins, outs):
        return [
            (ins[k].at[pl.ds((side ^ scalars[0]) * quad, quad)], outs[side].at[pl.ds(k * quad, quad)])
            for k in range(4)
            for side in range(2)
        ]

    keep, give = copied(core_plan, [c], lines, [(4 * quad, *tile)] * 2)
    got = permuted(give, lambda g, d: (g ^ 1, d))

    total = near + far
    total = jnp.stack([total, over_x(total, 1)])
    total = jnp.concatenate([total, over_x(total, 2)]).reshape(-1, col_dev)
    total = jnp.concatenate([total, *(over_y(total, k) for k in (1, 2, 3))])
    total = jnp.concatenate([total, permuted(total, lambda g, d: (g ^ 1, d))])
    scale = 1.0 / (rows_all * cols_all)
    coef = scale * lax.dot_general(total, pinv_f, (((0,), (0,)), ((), ())), precision=HIGH)[:modes]
    index = np.arange(FREQS)
    step = np.where(index < BAND, index, index - (BAND - 1))
    weight = np.where(step == 0, 1.0, 2.0)
    kmax = np.maximum(step[:, None], step[None, :]).reshape(-1)
    both = (weight[:, None] * weight[None, :]).reshape(-1).astype(np.float32)
    masked = jnp.where(jnp.asarray(kmax)[:, None] < bands[None, :], coef, 0.0)
    signed = jnp.dot(jnp.asarray(mirror()), masked, precision=HIGH)
    spectrum = signed.reshape(FREQS, FREQS, 2, solved).transpose(2, 3, 0, 1)
    weighed = masked * jnp.asarray(both)[:, None]
    row_here = basis(grp * row_dev + jnp.arange(row_dev, dtype=jnp.int32), rows_all)

    cut = 4 * quad
    first = [(keep, pinv_a[:, :cut], design_a[:cut]), (got, pinv_a[:, cut:], design_a[cut:])]
    images, misfits = [], []
    for part, pieces in enumerate((first, [(block, pinv, design)])):
        here = cols[part * span : (part + 1) * span]
        waves = row_here.T[:, None, :, None] * here.T[None, :, None, :]
        ramp = lax.dot_general(
            weighed, waves.reshape(modes, -1), (((0,), (0,)), ((), ())), precision=HIGH
        )
        series = 0.0
        for held_block, some_pinv, _ in pieces:
            flat = held_block.reshape(-1, row_dev * span)
            series = series + jnp.dot(some_pinv, flat, preferred_element_type=jnp.float32)
        image = (series - ramp).astype(jnp.bfloat16)
        images.append(image.reshape(solved, row_dev, span))
        energy = 0.0
        for held_block, _, some_design in pieces:
            flat = held_block.reshape(-1, row_dev * span)
            model = jnp.dot(
                some_design, series.astype(jnp.bfloat16), preferred_element_type=jnp.float32
            )
            resid = flat.astype(jnp.float32) - model
            energy = energy + jnp.sum(resid * resid, axis=0)
        misfit = jnp.sqrt(energy / ifgs + 1e-06)
        misfits.append(misfit.reshape(row_dev, span))
    return (jnp.concatenate(images, axis=2), jnp.concatenate(misfits, axis=1), spectrum)


def solution(mesh):
    return jax.shard_map(
        on_device,
        mesh=mesh,
        in_specs=(P("grp", None, "dev"), P(), P()),
        out_specs=(P(None, "grp", "dev"), P("grp", "dev"), P()),
        check_vma=False,
    )
```

```python
import functools
import math

import jax
import jax.numpy as jnp
import numpy as np
from jax import lax
from jax.experimental import pallas as pl
from jax.experimental.pallas import tpu as pltpu
from jax.sharding import PartitionSpec as P


BAND = 8
FREQS = 2 * BAND - 1
HIGH = lax.Precision.HIGHEST


def design_of(network, solved):
    dates = jnp.arange(1, solved + 1, dtype=jnp.int32)
    return (network[:, 1:2] == dates[None, :]).astype(jnp.float32) - (
        network[:, 0:1] == dates[None, :]
    ).astype(jnp.float32)


def sweep_kernel(normal_ref, out_ref):
    size, width = out_ref.shape
    out_ref[...] = normal_ref[...]
    lane = lax.broadcasted_iota(jnp.int32, (size, width), 1)
    top = lax.broadcasted_iota(jnp.int32, (1, width), 1)

    def pick(row, at):
        return jnp.sum(jnp.where(top == at, row, 0.0), axis=1, keepdims=True)

    def step(i, carry):
        k = 2 * i
        whole = out_ref[...]
        row0 = out_ref[pl.ds(k, 1), :]
        row1 = out_ref[pl.ds(k + 1, 1), :]
        first, second = lane == k, lane == k + 1
        col0 = jnp.sum(jnp.where(first, whole, 0.0), axis=1, keepdims=True)
        col1 = jnp.sum(jnp.where(second, whole, 0.0), axis=1, keepdims=True)
        p, q = pick(row0, k), pick(row0, k + 1)
        t, r = pick(row1, k), pick(row1, k + 1)
        inv = 1.0 / (p * r - q * t)
        row0 = jnp.where(top == k, 1.0, jnp.where(top == k + 1, 0.0, row0))
        row1 = jnp.where(top == k, 0.0, jnp.where(top == k + 1, 1.0, row1))
        new0 = (r * row0 - q * row1) * inv
        new1 = (p * row1 - t * row0) * inv
        rest = jnp.where(first | second, 0.0, whole)
        out_ref[...] = rest - col0 * new0 - col1 * new1
        out_ref[pl.ds(k, 1), :] = new0
        out_ref[pl.ds(k + 1, 1), :] = new1
        return carry

    lax.fori_loop(0, size // 2, step, 0)


def inverse_of(design):
    solved = design.shape[1]
    normal = lax.dot_general(
        design, design, (((0,), (0,)), ((), ())), preferred_element_type=jnp.float32
    )
    size, width = -(-solved // 8) * 8, -(-solved // 128) * 128
    padded = jnp.pad(normal, ((0, size - solved), (0, width - solved)))
    at = jnp.arange(size)
    ones = jnp.where(at >= solved, 1.0, 0.0).astype(jnp.float32)
    padded = padded + jnp.where(at[:, None] == jnp.arange(width)[None, :], ones[:, None], 0.0)
    inverse = pl.pallas_call(
        sweep_kernel,
        out_shape=jax.ShapeDtypeStruct((size, width), jnp.float32),
        in_specs=[pl.BlockSpec(memory_space=pltpu.VMEM)],
        out_specs=pl.BlockSpec(memory_space=pltpu.VMEM),
        cost_estimate=pl.CostEstimate(
            flops=int(3e7), bytes_accessed=300000, transcendentals=0
        ),
        compiler_params=pltpu.CompilerParams(vmem_limit_bytes=2 << 20),
        name="sweep",
    )(padded)
    return inverse[:solved, :solved]


def basis(positions, length):
    index = jnp.arange(FREQS, dtype=jnp.int32)
    step = jnp.where(index < BAND, index, index - (BAND - 1))
    turns = positions[:, None] * step[None, :] % length
    angle = turns.astype(jnp.float32) * (2.0 * math.pi / length)
    return jnp.where(index[None, :] < BAND, jnp.cos(angle), jnp.sin(angle))


def mirror():
    out = np.zeros((FREQS, FREQS, 2, FREQS, FREQS), np.float32)
    for k in range(FREQS):
        for l in range(FREQS):
            fk, fl = k - (BAND - 1), l - (BAND - 1)
            ck, cl = abs(fk), abs(fl)
            sk, sl = abs(fk) + BAND - 1, abs(fl) + BAND - 1
            gk, gl = np.sign(fk), np.sign(fl)
            out[k, l, 0, ck, cl] += 1
            if gk * gl:
                out[k, l, 0, sk, sl] -= gk * gl
            if gk:
                out[k, l, 1, sk, cl] -= gk
            if gl:
                out[k, l, 1, ck, sl] -= gl
    return out.reshape(FREQS * FREQS * 2, FREQS * FREQS)


DEVS = 8


def permuted(value, move):
    pairs = []
    for g in range(32):
        for d in range(DEVS):
            to_g, to_d = move(g, d)
            pairs.append((g * DEVS + d, to_g * DEVS + to_d))
    return lax.ppermute(value, ("grp", "dev"), pairs)


def over_y(value, k):
    return permuted(value, lambda g, d: (g ^ (k << 3), d))


def over_x(value, k):
    return permuted(value, lambda g, d: (g, d ^ (k << 1)))


def pack_kernel(part, strips_ref, out_ref, sems):
    held, span = out_ref.shape[1], out_ref.shape[3]
    copies = [
        pltpu.make_async_copy(
            strips_ref.at[i, :, :, pl.ds(part * span, span)], out_ref.at[:, i], sems.at[i]
        )
        for i in range(held)
    ]
    for copy in copies:
        copy.start()
    for copy in copies:
        copy.wait()


def pack(strips, part, span):
    held, groups, row_dev, _ = strips.shape
    return pl.pallas_call(
        functools.partial(pack_kernel, part),
        out_shape=jax.ShapeDtypeStruct((groups, held, row_dev, span), strips.dtype),
        in_specs=[pl.BlockSpec(memory_space=pl.ANY)],
        out_specs=pl.BlockSpec(memory_space=pltpu.VMEM),
        scratch_shapes=[pltpu.SemaphoreType.DMA((held,))],
    )(strips)


def on_device(stack, network, bands):
    solved = bands.shape[0]
    grp, dev = lax.axis_index("grp"), lax.axis_index("dev")
    y, z, c, x = grp // 8, grp // 2 % 4, grp % 2, dev // 2
    groups = lax.axis_size("grp")
    held, rows_all, col_dev = stack.shape
    row_dev = rows_all // groups
    cols_all = col_dev * lax.axis_size("dev")
    modes = FREQS * FREQS
    ifgs = held * groups
    span = col_dev // 2

    strips = stack.reshape(held, groups, row_dev, col_dev)
    blocks = []
    for part in range(2):
        packed = pack(strips, part, span)
        blocks.append(lax.all_to_all(packed, "grp", 0, 0, tiled=True))

    rows = basis(jnp.arange(rows_all, dtype=jnp.int32), rows_all)
    cols = basis(dev * col_dev + jnp.arange(col_dev, dtype=jnp.int32), cols_all)
    wide = stack.astype(jnp.float32)
    half = jnp.einsum("ihw,ha->iaw", wide, rows, precision=HIGH)
    local = jnp.einsum("iaw,wb->iab", half, cols, precision=HIGH)
    deep = -(-held // 8) * 8
    local = jnp.pad(local.reshape(held, modes), ((0, deep - held), (0, col_dev - modes)))
    local = local + over_x(local, 1)
    local = local + over_x(local, 2)
    near = permuted(local, lambda g, d: (g ^ (d // 2 << 1), d))
    far = permuted(local, lambda g, d: (g ^ (d // 2 << 1), d ^ 1))

    design = design_of(network, solved).astype(jnp.bfloat16)
    kc, ky, kr, j = np.meshgrid(
        np.arange(2), np.arange(4), np.arange(4), np.arange(deep), indexing="ij"
    )
    order = (((y ^ ky) * 4 + (z ^ x ^ kr)) * 2 + (c ^ kc)) * held + j
    order = jnp.where(j < held, order, -1).reshape(-1)
    inverse = inverse_of(design)
    pinv = lax.dot_general(
        inverse, design.astype(jnp.float32), (((1,), (1,)), ((), ())), precision=HIGH
    ).astype(jnp.bfloat16)
    chosen = (order[:, None] == jnp.arange(ifgs)[None, :]).astype(jnp.bfloat16)
    pinv_f = lax.dot_general(
        chosen, pinv, (((1,), (1,)), ((), ())), preferred_element_type=jnp.float32
    )

    total = near + far
    total = jnp.stack([total, over_x(total, 1)])
    total = jnp.concatenate([total, over_x(total, 2)]).reshape(-1, col_dev)
    lines = [over_y(total, k) for k in (1, 2, 3)]
    total = jnp.concatenate([total, *lines])
    other = permuted(total, lambda g, d: (g ^ 1, d))
    total = jnp.concatenate([total, other])

    scale = 1.0 / (rows_all * cols_all)
    coef = scale * lax.dot_general(total, pinv_f, (((0,), (0,)), ((), ())), precision=HIGH)[:modes]
    index = np.arange(FREQS)
    step = np.where(index < BAND, index, index - (BAND - 1))
    weight = np.where(step == 0, 1.0, 2.0)
    kmax = np.maximum(step[:, None], step[None, :]).reshape(-1)
    both = (weight[:, None] * weight[None, :]).reshape(-1).astype(np.float32)
    masked = jnp.where(jnp.asarray(kmax)[:, None] < bands[None, :], coef, 0.0)
    signed = jnp.dot(jnp.asarray(mirror()), masked, precision=HIGH)
    spectrum = signed.reshape(FREQS, FREQS, 2, solved).transpose(2, 3, 0, 1)
    weighed = masked * jnp.asarray(both)[:, None]
    row_here = basis(grp * row_dev + jnp.arange(row_dev, dtype=jnp.int32), rows_all)

    images, misfits = [], []
    for part, block in enumerate(blocks):
        here = cols[part * span : (part + 1) * span]
        waves = row_here.T[:, None, :, None] * here.T[None, :, None, :]
        ramp = lax.dot_general(
            weighed, waves.reshape(modes, -1), (((0,), (0,)), ((), ())), precision=HIGH
        )
        flat = block.reshape(ifgs, row_dev * span)
        series = jnp.dot(pinv, flat, preferred_element_type=jnp.float32)
        image = (series - ramp).astype(jnp.bfloat16)
        images.append(image.reshape(solved, row_dev, span))
        model = jnp.dot(
            design, series.astype(jnp.bfloat16), preferred_element_type=jnp.float32
        )
        resid = flat.astype(jnp.float32) - model
        misfit = jnp.sqrt(jnp.mean(resid * resid, axis=0) + 1e-06)
        misfits.append(misfit.reshape(row_dev, span))
    return (jnp.concatenate(images, axis=2), jnp.concatenate(misfits, axis=1), spectrum)


def solution(mesh):
    return jax.shard_map(
        on_device,
        mesh=mesh,
        in_specs=(P("grp", None, "dev"), P(), P()),
        out_specs=(P(None, "grp", "dev"), P("grp", "dev"), P()),
        check_vma=False,
    )
```

```python
import functools
import math

import jax
import jax.numpy as jnp
import numpy as np
from jax import lax
from jax.experimental import pallas as pl
from jax.experimental.pallas import tpu as pltpu
from jax.sharding import PartitionSpec as P


BAND = 8
FREQS = 2 * BAND - 1
HIGH = lax.Precision.HIGHEST


def design_of(network, solved):
    dates = jnp.arange(1, solved + 1, dtype=jnp.int32)
    return (network[:, 1:2] == dates[None, :]).astype(jnp.float32) - (
        network[:, 0:1] == dates[None, :]
    ).astype(jnp.float32)


def sweep_kernel(normal_ref, out_ref):
    size, width = out_ref.shape
    out_ref[...] = normal_ref[...]
    lane = lax.broadcasted_iota(jnp.int32, (size, width), 1)
    top = lax.broadcasted_iota(jnp.int32, (1, width), 1)

    def pick(row, at):
        return jnp.sum(jnp.where(top == at, row, 0.0), axis=1, keepdims=True)

    def step(i, carry):
        k = 2 * i
        whole = out_ref[...]
        row0 = out_ref[pl.ds(k, 1), :]
        row1 = out_ref[pl.ds(k + 1, 1), :]
        first, second = lane == k, lane == k + 1
        col0 = jnp.sum(jnp.where(first, whole, 0.0), axis=1, keepdims=True)
        col1 = jnp.sum(jnp.where(second, whole, 0.0), axis=1, keepdims=True)
        p, q = pick(row0, k), pick(row0, k + 1)
        t, r = pick(row1, k), pick(row1, k + 1)
        inv = 1.0 / (p * r - q * t)
        row0 = jnp.where(top == k, 1.0, jnp.where(top == k + 1, 0.0, row0))
        row1 = jnp.where(top == k, 0.0, jnp.where(top == k + 1, 1.0, row1))
        new0 = (r * row0 - q * row1) * inv
        new1 = (p * row1 - t * row0) * inv
        rest = jnp.where(first | second, 0.0, whole)
        out_ref[...] = rest - col0 * new0 - col1 * new1
        out_ref[pl.ds(k, 1), :] = new0
        out_ref[pl.ds(k + 1, 1), :] = new1
        return carry

    lax.fori_loop(0, size // 2, step, 0)


def inverse_of(design):
    solved = design.shape[1]
    normal = lax.dot_general(
        design, design, (((0,), (0,)), ((), ())), preferred_element_type=jnp.float32
    )
    size, width = -(-solved // 8) * 8, -(-solved // 128) * 128
    padded = jnp.pad(normal, ((0, size - solved), (0, width - solved)))
    at = jnp.arange(size)
    ones = jnp.where(at >= solved, 1.0, 0.0).astype(jnp.float32)
    padded = padded + jnp.where(at[:, None] == jnp.arange(width)[None, :], ones[:, None], 0.0)
    inverse = pl.pallas_call(
        sweep_kernel,
        out_shape=jax.ShapeDtypeStruct((size, width), jnp.float32),
        in_specs=[pl.BlockSpec(memory_space=pltpu.VMEM)],
        out_specs=pl.BlockSpec(memory_space=pltpu.VMEM),
        cost_estimate=pl.CostEstimate(
            flops=int(3e7), bytes_accessed=300000, transcendentals=0
        ),
        compiler_params=pltpu.CompilerParams(vmem_limit_bytes=2 << 20),
        name="sweep",
    )(padded)
    return inverse[:solved, :solved]


def basis(positions, length):
    index = jnp.arange(FREQS, dtype=jnp.int32)
    step = jnp.where(index < BAND, index, index - (BAND - 1))
    turns = positions[:, None] * step[None, :] % length
    angle = turns.astype(jnp.float32) * (2.0 * math.pi / length)
    return jnp.where(index[None, :] < BAND, jnp.cos(angle), jnp.sin(angle))


def mirror():
    out = np.zeros((FREQS, FREQS, 2, FREQS, FREQS), np.float32)
    for k in range(FREQS):
        for l in range(FREQS):
            fk, fl = k - (BAND - 1), l - (BAND - 1)
            ck, cl = abs(fk), abs(fl)
            sk, sl = abs(fk) + BAND - 1, abs(fl) + BAND - 1
            gk, gl = np.sign(fk), np.sign(fl)
            out[k, l, 0, ck, cl] += 1
            if gk * gl:
                out[k, l, 0, sk, sl] -= gk * gl
            if gk:
                out[k, l, 1, sk, cl] -= gk
            if gl:
                out[k, l, 1, ck, sl] -= gl
    return out.reshape(FREQS * FREQS * 2, FREQS * FREQS)


DEVS = 8


def permuted(value, move):
    pairs = []
    for g in range(32):
        for d in range(DEVS):
            to_g, to_d = move(g, d)
            pairs.append((g * DEVS + d, to_g * DEVS + to_d))
    return lax.ppermute(value, ("grp", "dev"), pairs)


def over_y(value, k):
    return permuted(value, lambda g, d: (g ^ (k << 3), d))


def over_x(value, k):
    return permuted(value, lambda g, d: (g, d ^ (k << 1)))


def pack_kernel(part, strips_ref, out_ref, buffer, in_sems, out_sems):
    groups, _, _, span = out_ref.shape
    reads = [
        pltpu.make_async_copy(
            strips_ref.at[:, j, :, pl.ds(part * span, span)], buffer.at[j], in_sems.at[j]
        )
        for j in range(groups)
    ]
    writes = [
        pltpu.make_async_copy(buffer.at[j], out_ref.at[j], out_sems.at[j])
        for j in range(groups)
    ]
    for read in reads:
        read.start()
    for read, write in zip(reads, writes):
        read.wait()
        write.start()
    for write in writes:
        write.wait()


def pack(strips, part, span):
    held, groups, row_dev, _ = strips.shape
    shape = (groups, held, row_dev, span)
    return pl.pallas_call(
        functools.partial(pack_kernel, part),
        out_shape=jax.ShapeDtypeStruct(shape, strips.dtype),
        in_specs=[pl.BlockSpec(memory_space=pl.ANY)],
        out_specs=pl.BlockSpec(memory_space=pl.ANY),
        scratch_shapes=[
            pltpu.VMEM(shape, strips.dtype),
            pltpu.SemaphoreType.DMA((groups,)),
            pltpu.SemaphoreType.DMA((groups,)),
        ],
    )(strips)


def on_device(stack, network, bands):
    solved = bands.shape[0]
    grp, dev = lax.axis_index("grp"), lax.axis_index("dev")
    y, z, c, x = grp // 8, grp // 2 % 4, grp % 2, dev // 2
    groups = lax.axis_size("grp")
    held, rows_all, col_dev = stack.shape
    row_dev = rows_all // groups
    cols_all = col_dev * lax.axis_size("dev")
    modes = FREQS * FREQS
    ifgs = held * groups
    span = col_dev // 2

    strips = stack.reshape(held, groups, row_dev, col_dev)
    blocks = []
    for part in range(2):
        packed = pack(strips, part, span)
        blocks.append(lax.all_to_all(packed, "grp", 0, 0, tiled=True))

    rows = basis(jnp.arange(rows_all, dtype=jnp.int32), rows_all)
    cols = basis(dev * col_dev + jnp.arange(col_dev, dtype=jnp.int32), cols_all)
    wide = stack.astype(jnp.float32)
    half = jnp.einsum("ihw,ha->iaw", wide, rows, precision=HIGH)
    local = jnp.einsum("iaw,wb->iab", half, cols, precision=HIGH)
    deep = -(-held // 8) * 8
    local = jnp.pad(local.reshape(held, modes), ((0, deep - held), (0, col_dev - modes)))
    local = local + over_x(local, 1)
    local = local + over_x(local, 2)
    near = permuted(local, lambda g, d: (g ^ (d // 2 << 1), d))
    far = permuted(local, lambda g, d: (g ^ (d // 2 << 1), d ^ 1))

    design = design_of(network, solved).astype(jnp.bfloat16)
    kc, ky, kr, j = np.meshgrid(
        np.arange(2), np.arange(4), np.arange(4), np.arange(deep), indexing="ij"
    )
    order = (((y ^ ky) * 4 + (z ^ x ^ kr)) * 2 + (c ^ kc)) * held + j
    order = jnp.where(j < held, order, -1).reshape(-1)
    inverse = inverse_of(design)
    pinv = lax.dot_general(
        inverse, design.astype(jnp.float32), (((1,), (1,)), ((), ())), precision=HIGH
    ).astype(jnp.bfloat16)
    chosen = (order[:, None] == jnp.arange(ifgs)[None, :]).astype(jnp.bfloat16)
    pinv_f = lax.dot_general(
        chosen, pinv, (((1,), (1,)), ((), ())), preferred_element_type=jnp.float32
    )

    total = near + far
    total = jnp.stack([total, over_x(total, 1)])
    total = jnp.concatenate([total, over_x(total, 2)]).reshape(-1, col_dev)
    lines = [over_y(total, k) for k in (1, 2, 3)]
    total = jnp.concatenate([total, *lines])
    other = permuted(total, lambda g, d: (g ^ 1, d))
    total = jnp.concatenate([total, other])

    scale = 1.0 / (rows_all * cols_all)
    coef = scale * lax.dot_general(total, pinv_f, (((0,), (0,)), ((), ())), precision=HIGH)[:modes]
    index = np.arange(FREQS)
    step = np.where(index < BAND, index, index - (BAND - 1))
    weight = np.where(step == 0, 1.0, 2.0)
    kmax = np.maximum(step[:, None], step[None, :]).reshape(-1)
    both = (weight[:, None] * weight[None, :]).reshape(-1).astype(np.float32)
    masked = jnp.where(jnp.asarray(kmax)[:, None] < bands[None, :], coef, 0.0)
    signed = jnp.dot(jnp.asarray(mirror()), masked, precision=HIGH)
    spectrum = signed.reshape(FREQS, FREQS, 2, solved).transpose(2, 3, 0, 1)
    weighed = masked * jnp.asarray(both)[:, None]
    row_here = basis(grp * row_dev + jnp.arange(row_dev, dtype=jnp.int32), rows_all)

    images, misfits = [], []
    for part, block in enumerate(blocks):
        here = cols[part * span : (part + 1) * span]
        waves = row_here.T[:, None, :, None] * here.T[None, :, None, :]
        ramp = lax.dot_general(
            weighed, waves.reshape(modes, -1), (((0,), (0,)), ((), ())), precision=HIGH
        )
        flat = block.reshape(ifgs, row_dev * span)
        if part:
            ramp = lax.optimization_barrier(ramp)
        series = jnp.dot(pinv, flat, preferred_element_type=jnp.float32)
        image = (series - ramp).astype(jnp.bfloat16)
        images.append(image.reshape(solved, row_dev, span))
        model = jnp.dot(
            design, series.astype(jnp.bfloat16), preferred_element_type=jnp.float32
        )
        resid = flat.astype(jnp.float32) - model
        misfit = jnp.sqrt(jnp.mean(resid * resid, axis=0) + 1e-06)
        misfits.append(misfit.reshape(row_dev, span))
    return (jnp.concatenate(images, axis=2), jnp.concatenate(misfits, axis=1), spectrum)


def solution(mesh):
    return jax.shard_map(
        on_device,
        mesh=mesh,
        in_specs=(P("grp", None, "dev"), P(), P()),
        out_specs=(P(None, "grp", "dev"), P("grp", "dev"), P()),
        check_vma=False,
    )
```
